64 devices in a mesh: dp: 8 (over x, y, core), tp: 8 (over z).
Axes of the slice: x: 2, y: 2, z: 8, core: 2. Of those that a mesh axis runs over, the one named last changes fastest.
The devices are a block of a 4x4x8 slice.
Arguments:
- x: bfloat16 [512, 2048], P('dp'), parts along dimension 0
- k_cache: bfloat16 [512, 1024, 16, 128], P('dp', None, 'tp'), parts along dimension 0
- v_cache: bfloat16 [512, 1024, 16, 128], P('dp', None, 'tp'), parts along dimension 0
- gain_a: bfloat16 [2048], replicated
- wq: bfloat16 [2048, 2048], P(None, 'tp')
- wo: bfloat16 [2048, 2048], P('tp')
- gain_m: bfloat16 [2048], replicated
- w_gate: bfloat16 [2048, 8192], P(None, 'tp')
- w_up: bfloat16 [2048, 8192], P(None, 'tp')
- w_down: bfloat16 [8192, 2048], P('tp')
Outputs:
- output: bfloat16 [512, 2048], P('dp'), parts along dimension 0
There are 8 independent parts. The reference program is written for one: setup_inputs(seed, part) draws one part's arguments, and reference() takes and returns one part's arrays. A program takes and returns all parts, laid end to end along the dimension named above; an argument that names none is the same for every part.
All inputs are finite; a program needn't handle non-finite values.
Results may differ from the reference program's by a relative error of at most 0.017.
Values are sent between devices in bfloat16 or wider.
A program may use at most 768 MiB of HBM per device.

```python
import jax
import jax.numpy as jnp
from jax import lax

BATCH = 64
CACHE = 1024
D = 2048
HEADS = 16
KV_HEADS = 16
HEAD = 128
FF = 8192
THETA = 10000


def setup_inputs(seed: int = 0, part: int = 0) -> dict:
    kx, kc, kw, kn, kq, ko, km, kg, ku, kd = jax.random.split(jax.random.key(seed), 10)
    kx, kc, kw = (jax.random.fold_in(k, part) for k in (kx, kc, kw))

    def weights(key, rows, columns):
        return jax.random.normal(key, (rows, columns), jnp.float32) * rows**-0.5

    drawn = {
        "x": jax.random.normal(kx, (BATCH, D), jnp.float32),
        "k_cache": 2 * jax.random.normal(kc, (BATCH, CACHE, KV_HEADS, HEAD), jnp.float32),
        "v_cache": 4 * jax.random.normal(kw, (BATCH, CACHE, KV_HEADS, HEAD), jnp.float32),
        "gain_a": 1 + 0.1 * jax.random.normal(kn, (D,), jnp.float32),
        "wq": 2 * weights(kq, D, HEADS * HEAD),
        "wo": weights(ko, HEADS * HEAD, D),
        "gain_m": 1 + 0.1 * jax.random.normal(km, (D,), jnp.float32),
        "w_gate": weights(kg, D, FF),
        "w_up": weights(ku, D, FF),
        "w_down": 2 * weights(kd, FF, D),
    }
    return {k: v.astype(jnp.bfloat16) for k, v in drawn.items()}


def normed(x, gain):
    wide = x.astype(jnp.float32)
    scale = lax.rsqrt(jnp.mean(wide * wide, -1, keepdims=True) + 1e-6)
    return (wide * scale * gain.astype(jnp.float32)).astype(jnp.bfloat16)


def turned(t, place, theta):
    half = t.shape[-1] // 2
    angle = place.astype(jnp.float32)[:, None] * theta ** (-jnp.arange(half, dtype=jnp.float32) / half)
    cos, sin = jnp.cos(angle)[:, None], jnp.sin(angle)[:, None]
    a, b = t[..., :half].astype(jnp.float32), t[..., half:].astype(jnp.float32)
    return jnp.concatenate([a * cos - b * sin, b * cos + a * sin], -1).astype(jnp.bfloat16)


def matmul(a, w):
    return jnp.dot(a, w, preferred_element_type=jnp.float32).astype(jnp.bfloat16)


def einsum(form, a, b):
    return jnp.einsum(form, a.astype(jnp.float32), b.astype(jnp.float32))


def seen_by(a, wq, k_cache, v_cache, head, theta):
    batch, cache, kv_heads = k_cache.shape[:3]
    place = jnp.full((batch,), cache - 1)
    q = turned(matmul(a, wq).reshape(batch, -1, head), place, theta).reshape(batch, kv_heads, -1, head)
    scores = einsum("bgsd,bugd->bgsu", q, k_cache) * head**-0.5
    weights = jax.nn.softmax(scores, -1).astype(jnp.bfloat16)
    return einsum("bgsu,bugd->bgsd", weights, v_cache).astype(jnp.bfloat16).reshape(batch, -1)


def hidden_of(b, w_gate, w_up):
    gate = jnp.dot(b, w_gate, preferred_element_type=jnp.float32)
    up = jnp.dot(b, w_up, preferred_element_type=jnp.float32)
    return (jax.nn.silu(gate) * up).astype(jnp.bfloat16)


def reference(x, k_cache, v_cache, gain_a, wq, wo, gain_m, w_gate, w_up, w_down):
    seen = seen_by(normed(x, gain_a), wq, k_cache, v_cache, HEAD, THETA)
    h = (x.astype(jnp.float32) + jnp.dot(seen, wo, preferred_element_type=jnp.float32)).astype(jnp.bfloat16)
    hidden = hidden_of(normed(h, gain_m), w_gate, w_up)
    return (h.astype(jnp.float32) + jnp.dot(hidden, w_down, preferred_element_type=jnp.float32)).astype(jnp.bfloat16)
```

```python
import functools

import jax
import jax.numpy as jnp
import numpy as np
from jax import lax
from jax.experimental import pallas as pl
from jax.experimental.pallas import tpu as pltpu
from jax.sharding import PartitionSpec as P

HEAD = 128
THETA = 10000
F32, BF16 = jnp.float32, jnp.bfloat16

CH = 8
SLOTS = 4
LAG = 3


def dot(a, b):
    return lax.dot_general(a, b, (((1,), (0,)), ((), ())), preferred_element_type=F32)


def dot_t(a, b):
    return lax.dot_general(a, b, (((1,), (1,)), ((), ())), preferred_element_type=F32)


def kernel(n, x_hbm, k_hbm, v_hbm, ga_hbm, wq_hbm, wo_hbm, gm_hbm, wg_hbm, wu_hbm, wd_hbm, cs_hbm, y_ref,
           xb, xf, ga, gm, cs, wq, wo, wg, wu, wd, kbuf, vbuf, qf, pf, sbuf, rbuf, hbuf, bbuf, p2, s2, r2, ybuf,
           sem_in, sem_k, sem_v, rs_s, rs_r, ag_s, ag_r, rs2_s, rs2_r, ag2_s, ag2_r):
    me = lax.axis_index("tp")
    rows, d = xb.shape
    chunks = rows // CH
    blk = d // n
    span = kbuf.shape[2] // 2

    def peer(j):
        return lax.rem(me + j, n)

    def load(i, src, dst):
        return pltpu.make_async_copy(src, dst, sem_in.at[i])

    first = [load(0, x_hbm, xb), load(1, ga_hbm, ga), load(2, cs_hbm, cs), load(3, wq_hbm, wq)]
    second = [load(4, wo_hbm, wo), load(5, gm_hbm, gm)]
    third = [load(6, wg_hbm, wg), load(7, wu_hbm, wu), load(8, wd_hbm, wd)]

    def fetch_k(c, slot):
        return pltpu.make_async_copy(k_hbm.at[pl.ds(c * CH, CH)], kbuf.at[slot], sem_k.at[slot])

    def fetch_v(c, slot):
        return pltpu.make_async_copy(v_hbm.at[pl.ds(c * CH, CH)], vbuf.at[slot], sem_v.at[slot])

    for cp in first:
        cp.start()
    fetch_k(0, 0).start()
    fetch_v(0, 0).start()
    for cp in second:
        cp.start()
    for c in range(1, SLOTS):
        fetch_k(c, c).start()
        fetch_v(c, c).start()

    barrier = pltpu.get_barrier_semaphore()
    for j in range(1, n):
        pl.semaphore_signal(barrier, inc=1, device_id={"tp": peer(j)})

    for cp in first[:3]:
        cp.wait()
    xv = xb[...].astype(F32)
    xf[...] = xv
    scale = lax.rsqrt(jnp.sum(xv * xv, -1, keepdims=True) * (1.0 / d) + 1e-6)
    gav = ga[...].astype(F32)
    for i in range(d // 128):
        at = slice(128 * i, 128 * i + 128)
        bbuf[:, at] = (xf[:, at] * scale * gav[i:i + 1]).astype(BF16)
    first[3].wait()
    q = dot(bbuf[...], wq[...]).astype(BF16).astype(F32)
    for g in range(2):
        t = q[:, HEAD * g:HEAD * (g + 1)]
        turned = t * cs[0:1] + pltpu.roll(t, HEAD // 2, 1) * cs[1:2]
        qf[:, HEAD * g:HEAD * (g + 1)] = turned.astype(BF16).astype(F32)

    for cp in second:
        cp.wait()
    pl.semaphore_wait(barrier, n - 1)

    def rs_copy(c, j):
        return pltpu.make_async_remote_copy(
            src_ref=sbuf.at[c, peer(j)], dst_ref=rbuf.at[c, j - 1], send_sem=rs_s.at[c], recv_sem=rs_r.at[c],
            device_id={"tp": peer(j)})

    def ag_copy(c, j):
        return pltpu.make_async_remote_copy(
            src_ref=hbuf.at[c, me], dst_ref=hbuf.at[c, me], send_sem=ag_s.at[c], recv_sem=ag_r.at[c],
            device_id={"tp": peer(j)})

    def all_of(ref, sem):
        pltpu.make_async_copy(ref, ref, sem).wait()

    def finish(c):
        all_of(rbuf.at[c], rs_r.at[c])
        total = pf[c, me]
        for j in range(n - 1):
            total = total + rbuf[c, j].astype(F32)
        total = total + xf[pl.ds(pl.multiple_of(c * CH, CH), CH), pl.ds(pl.multiple_of(me * blk, blk), blk)]
        hbuf[c, me] = total.astype(BF16)
        for j in range(1, n):
            ag_copy(c, j).start()

    row = lax.broadcasted_iota(jnp.int32, (4 * CH, 256), 0)
    row_w = lax.broadcasted_iota(jnp.int32, (4 * CH, span), 0)
    col_w = lax.broadcasted_iota(jnp.int32, (4 * CH, span), 1)
    seen_by_row = (col_w % 2) == ((row_w // CH) % 2)

    def attend(c, _):
        slot = lax.rem(c, SLOTS)
        fetch_k(c, slot).wait()
        qc = qf[pl.ds(pl.multiple_of(c * CH, CH), CH), :]
        q0, q1 = qc[:, :HEAD], qc[:, HEAD:]
        zero = jnp.zeros_like(q0)
        base = jnp.concatenate([jnp.concatenate([q0, q1, zero, zero], 0), jnp.concatenate([zero, zero, q0, q1], 0)], 1)
        s = None
        for i in range(CH):
            lhs = jnp.where(row % CH == i, base, 0.0).astype(BF16)
            keys = jnp.concatenate([kbuf[slot, i, :span], kbuf[slot, i, span:]], 1)
            t = dot_t(lhs, keys)
            s = t if s is None else s + t
        s = jnp.where(seen_by_row, s * HEAD**-0.5, -jnp.inf)
        m = jnp.max(s, -1, keepdims=True)
        m = jnp.maximum(m[:2 * CH], m[2 * CH:])
        m = jnp.concatenate([m, m], 0)
        e = jnp.exp(s - m)
        z = jnp.sum(e, -1, keepdims=True)
        z = z[:2 * CH] + z[2 * CH:]
        z = 1.0 / jnp.concatenate([z, z], 0)
        w = e * z
        fetch_v(c, slot).wait()
        o = None
        for i in range(CH):
            lhs = jnp.where(row_w % CH == i, w, 0.0).astype(BF16)
            values = jnp.concatenate([vbuf[slot, i, :span], vbuf[slot, i, span:]], 1)
            t = dot(lhs, values)
            o = t if o is None else o + t
        o = o[:2 * CH, :HEAD] + o[2 * CH:, HEAD:]
        seen = jnp.concatenate([o[:CH], o[CH:]], 1).astype(BF16)

        @pl.when(c + SLOTS < chunks)
        def _():
            fetch_k(c + SLOTS, slot).start()
            fetch_v(c + SLOTS, slot).start()

        @pl.when(c + SLOTS == chunks)
        def _():
            for cp in third:
                cp.start()

        term = dot(seen, wo[...])
        for j in range(n):
            part = term[:, blk * j:blk * (j + 1)]
            pf[c, j] = part
            sbuf[c, j] = part.astype(BF16)
        for j in range(1, n):
            rs_copy(c, j).start()

        @pl.when(c >= LAG)
        def _():
            finish(c - LAG)

        return 0

    lax.fori_loop(0, chunks, attend, 0)
    for c in range(chunks - LAG, chunks):
        finish(c)
    for cp in third:
        cp.wait()

    for c in range(chunks):
        all_of(rbuf.at[c], ag_r.at[c])
    gmv = gm[...].astype(F32)

    def h_block(j):
        return hbuf[:, j].astype(F32).reshape(rows, blk)

    total = None
    for j in range(n):
        hj = h_block(j)
        t = jnp.sum(hj * hj, -1, keepdims=True)
        total = t if total is None else total + t
    scale = lax.rsqrt(total * (1.0 / d) + 1e-6)
    for j in range(n):
        hj = h_block(j)
        for i in range(blk // 128):
            g = j * (blk // 128) + i
            bbuf[:, 128 * g:128 * g + 128] = (hj[:, 128 * i:128 * i + 128] * scale * gmv[g:g + 1]).astype(BF16)
    hidden = []
    for f in range(wg.shape[1] // 256):
        at = slice(256 * f, 256 * f + 256)
        gate = dot(bbuf[...], wg[:, at])
        up = dot(bbuf[...], wu[:, at])
        hidden.append((jax.nn.silu(gate) * up).astype(BF16))
    hidden = jnp.concatenate(hidden, 1)

    def rs2_copy(j):
        return pltpu.make_async_remote_copy(
            src_ref=s2.at[peer(j)], dst_ref=r2.at[j - 1], send_sem=rs2_s, recv_sem=rs2_r, device_id={"tp": peer(j)})

    def ag2_copy(j):
        return pltpu.make_async_remote_copy(
            src_ref=ybuf.at[me], dst_ref=ybuf.at[me], send_sem=ag2_s, recv_sem=ag2_r, device_id={"tp": peer(j)})

    for j in range(n):
        part = dot(hidden, wd[:, blk * j:blk * (j + 1)])
        p2[j] = part
        s2[j] = part.astype(BF16)
    for j in range(1, n):
        rs2_copy(j).start()
    all_of(r2, rs2_r)
    total = p2[me]
    for j in range(n - 1):
        total = total + r2[j].astype(F32)
    total = total + hbuf[:, me].astype(F32).reshape(rows, blk)
    ybuf[me] = total.astype(BF16)
    for j in range(1, n):
        ag2_copy(j).start()
    for c in range(chunks):
        all_of(rbuf.at[c], rs_s.at[c])
        all_of(rbuf.at[c], ag_s.at[c])
    all_of(r2, rs2_s)
    all_of(r2, ag2_r)
    all_of(r2, ag2_s)
    for j in range(n):
        y_ref[:, blk * j:blk * (j + 1)] = ybuf[j]


def solution(mesh):
    n = mesh.shape["tp"]

    def step(x, k_cache, v_cache, gain_a, wq, wo, gain_m, w_gate, w_up, w_down):
        rows, d = x.shape
        batch, cache, heads, head = k_cache.shape
        ff = w_gate.shape[1]
        chunks, blk = rows // CH, d // n
        half = head // 2
        angle = (cache - 1) * float(THETA) ** (-np.arange(half) / half)
        cos, sin = np.cos(angle), np.sin(angle)
        cs = np.zeros((8, head), np.float32)
        cs[0], cs[1] = np.concatenate([cos, cos]), np.concatenate([-sin, sin])
        keys = k_cache.reshape(batch, cache * heads, head)
        values = v_cache.reshape(batch, cache * heads, head)
        dma = pltpu.SemaphoreType.DMA
        return pl.pallas_call(
            functools.partial(kernel, n),
            out_shape=jax.ShapeDtypeStruct((rows, d), BF16),
            in_specs=[pl.BlockSpec(memory_space=pl.ANY)] * 11,
            out_specs=pl.BlockSpec(memory_space=pltpu.VMEM),
            scratch_shapes=[
                pltpu.VMEM((rows, d), BF16),
                pltpu.VMEM((rows, d), F32),
                pltpu.VMEM((d // 128, 128), BF16),
                pltpu.VMEM((d // 128, 128), BF16),
                pltpu.VMEM((8, head), F32),
                pltpu.VMEM(wq.shape, BF16),
                pltpu.VMEM(wo.shape, BF16),
                pltpu.VMEM(w_gate.shape, BF16),
                pltpu.VMEM(w_up.shape, BF16),
                pltpu.VMEM(w_down.shape, BF16),
                pltpu.VMEM((SLOTS, CH, cache * heads, head), BF16),
                pltpu.VMEM((SLOTS, CH, cache * heads, head), BF16),
                pltpu.VMEM((rows, heads * head), F32),
                pltpu.VMEM((chunks, n, CH, blk), F32),
                pltpu.VMEM((chunks, n, CH, blk), BF16),
                pltpu.VMEM((chunks, n - 1, CH, blk), BF16),
                pltpu.VMEM((chunks, n, CH, blk), BF16),
                pltpu.VMEM((rows, d), BF16),
                pltpu.VMEM((n, rows, blk), F32),
                pltpu.VMEM((n, rows, blk), BF16),
                pltpu.VMEM((n - 1, rows, blk), BF16),
                pltpu.VMEM((n, rows, blk), BF16),
                dma((9,)), dma((SLOTS,)), dma((SLOTS,)),
                dma((chunks,)), dma((chunks,)), dma((chunks,)), dma((chunks,)),
                dma(()), dma(()), dma(()), dma(()),
            ],
            compiler_params=pltpu.CompilerParams(
                collective_id=0, has_side_effects=True, vmem_limit_bytes=64 * 1024 * 1024 - 65536),
            name="decoder_layer",
        )(x, keys, values, gain_a.reshape(d // 128, 128), wq, wo, gain_m.reshape(d // 128, 128), w_gate, w_up, w_down, jnp.asarray(cs))

    states, cache, columns, rows_of = P("dp", None), P("dp", None, "tp", None), P(None, "tp"), P("tp", None)
    return jax.shard_map(
        step,
        mesh=mesh,
        in_specs=(states, cache, cache, P(None), columns, rows_of, P(None), columns, columns, rows_of),
        out_specs=states,
        check_vma=False,
    )
```

```python
import functools

import jax
import jax.numpy as jnp
import numpy as np
from jax import lax
from jax.experimental import pallas as pl
from jax.experimental.pallas import tpu as pltpu
from jax.sharding import PartitionSpec as P

HEAD = 128
THETA = 10000
F32, BF16 = jnp.float32, jnp.bfloat16

CH = 8
SLOTS = 3
LAG = 2
GROUP = 4
PASSES = (4, 3, 1)


def dot(a, b):
    return lax.dot_general(a, b, (((1,), (0,)), ((), ())), preferred_element_type=F32)


def dot_t(a, b):
    return lax.dot_general(a, b, (((1,), (1,)), ((), ())), preferred_element_type=F32)


def kernel(n, x_hbm, k_hbm, v_hbm, ga_hbm, wq_hbm, wo_hbm, gm_hbm, wg_hbm, wu_hbm, wd_hbm, cs_hbm, y_ref,
           xb, xf, ga, gm, cs, wq, wo, wg, wu, wd, kbuf, vbuf, qf, wbuf, pf, sbuf, rbuf, hbuf, bbuf, *rest):
    passes, (sem_in, sem_k, sem_v, rs_s, rs_r, ag_s, ag_r, rs2_s, rs2_r, ag2_s, ag2_r) = rest[:-11], rest[-11:]
    me = lax.axis_index("tp")
    rows, d = xb.shape
    chunks = rows // CH
    blk = d // n
    span = kbuf.shape[2] // 2

    far_first = sorted(range(1, n), key=lambda j: -min(j, n - j))

    def peer(j):
        return lax.rem(me + j, n)

    def load(i, src, dst):
        return pltpu.make_async_copy(src, dst, sem_in.at[i])

    first = [load(0, x_hbm, xb), load(1, ga_hbm, ga), load(2, cs_hbm, cs), load(3, wq_hbm, wq)]
    second = [load(4, wo_hbm, wo), load(5, gm_hbm, gm)]
    third = [load(6, wg_hbm, wg), load(7, wu_hbm, wu), load(8, wd_hbm, wd)]

    def fetch(hbm, buf, sem, c):
        slot = lax.rem(c, SLOTS)
        return pltpu.make_async_copy(hbm.at[pl.ds(c * CH, CH)], buf.at[slot], sem.at[slot])

    def fetch_k(c):
        return fetch(k_hbm, kbuf, sem_k, c)

    def fetch_v(c):
        return fetch(v_hbm, vbuf, sem_v, c)

    with jax.named_scope("start"):
        for cp in first:
            cp.start()
        fetch_k(0).start()
        barrier = pltpu.get_barrier_semaphore()
        for j in range(1, n):
            pl.semaphore_signal(barrier, inc=1, device_id={"tp": peer(j)})

    with jax.named_scope("wait_x"):
        for cp in first[:3]:
            cp.wait()
    with jax.named_scope("norm"):
        fetch_v(0).start()
        for cp in second:
            cp.start()
        fetch_k(1).start()
        xv = xb[...].astype(F32)
        xf[...] = xv
        scale = lax.rsqrt(jnp.sum(xv * xv, -1, keepdims=True) * (1.0 / d) + 1e-6)
        gav = ga[...].astype(F32)
        for i in range(d // 128):
            at = slice(128 * i, 128 * i + 128)
            bbuf[:, at] = (xf[:, at] * scale * gav[i:i + 1]).astype(BF16)
    with jax.named_scope("wait_wq"):
        first[3].wait()
        fetch_v(1).start()
    with jax.named_scope("qproj"):
        q = dot(bbuf[...], wq[...]).astype(BF16).astype(F32)
        for g in range(2):
            t = q[:, HEAD * g:HEAD * (g + 1)]
            turned = (t * cs[0:1] + pltpu.roll(t, HEAD // 2, 1) * cs[1:2]).astype(BF16).astype(F32)
            for i in range(rows // GROUP):
                qf[i, GROUP * g:GROUP * (g + 1)] = turned[GROUP * i:GROUP * (i + 1)]

    def rs_copy(c, j):
        return pltpu.make_async_remote_copy(
            src_ref=sbuf.at[c, peer(j)], dst_ref=rbuf.at[c, j - 1], send_sem=rs_s.at[c], recv_sem=rs_r.at[c],
            device_id={"tp": peer(j)})

    def ag_copy(c, j):
        return pltpu.make_async_remote_copy(
            src_ref=hbuf.at[c, me], dst_ref=hbuf.at[c, me], send_sem=ag_s.at[c], recv_sem=ag_r.at[c],
            device_id={"tp": peer(j)})

    def all_of(ref, sem):
        pltpu.make_async_copy(ref, ref, sem).wait()

    def finish(c):
        with jax.named_scope("finish_wait"):
            all_of(rbuf.at[c], rs_r.at[c])
        with jax.named_scope("finish"):
            total = pf[c, me]
            for j in range(n - 1):
                total = total + rbuf[c, j].astype(F32)
            total = total + xf[pl.ds(pl.multiple_of(c * CH, CH), CH), pl.ds(pl.multiple_of(me * blk, blk), blk)]
            hbuf[c, me] = total.astype(BF16)
            for j in far_first:
                ag_copy(c, j).start()

    tall = 4 * GROUP
    row = lax.broadcasted_iota(jnp.int32, (tall, 2 * HEAD), 0)
    row_w = lax.broadcasted_iota(jnp.int32, (tall, span), 0)
    col_w = lax.broadcasted_iota(jnp.int32, (tall, span), 1)
    own_head = (col_w % 2) == ((row_w // GROUP) % 2)
    groups = CH // GROUP

    def scored(c, g):
        slot = lax.rem(c, SLOTS)
        qg = qf[c * groups + g]
        zero = jnp.zeros_like(qg)
        base = jnp.concatenate([jnp.concatenate([qg, zero], 1), jnp.concatenate([zero, qg], 1)], 0)
        s = None
        for i in range(GROUP):
            lhs = jnp.where(row % GROUP == i, base, 0.0).astype(BF16)
            at = g * GROUP + i
            t = dot_t(lhs, jnp.concatenate([kbuf[slot, at, :span], kbuf[slot, at, span:]], 1))
            s = t if s is None else s + t
        return s

    def softmaxed(s):
        half = tall // 2
        s = jnp.where(own_head, s * HEAD**-0.5, -jnp.inf)
        m = jnp.max(s, -1, keepdims=True)
        m = jnp.maximum(m[:half], m[half:])
        e = jnp.exp(s - jnp.concatenate([m, m], 0))
        z = jnp.sum(e, -1, keepdims=True)
        z = 1.0 / (z[:half] + z[half:])
        return e * jnp.concatenate([z, z], 0)

    def mixed(c, g, w):
        slot = lax.rem(c, SLOTS)
        o = None
        for i in range(GROUP):
            lhs = jnp.where(row_w % GROUP == i, w, 0.0).astype(BF16)
            at = g * GROUP + i
            t = dot(lhs, jnp.concatenate([vbuf[slot, at, :span], vbuf[slot, at, span:]], 1))
            o = t if o is None else o + t
        return o[:tall // 2, :HEAD] + o[tall // 2:, HEAD:]

    def project(c, o):
        upper = lax.broadcasted_iota(jnp.int32, (CH, HEAD), 0) < GROUP
        head0 = jnp.where(upper, o[0], pltpu.roll(o[1], GROUP, 0))
        head1 = jnp.where(upper, pltpu.roll(o[0], GROUP, 0), o[1])
        seen = jnp.concatenate([head0, head1], 1).astype(BF16)
        term = dot(seen, wo[...])
        for j in range(n):
            part = term[:, blk * j:blk * (j + 1)]
            pf[c, j] = part
            sbuf[c, j] = part.astype(BF16)

    def send(c):
        for j in far_first:
            rs_copy(c, j).start()

    with jax.named_scope("k_wait"):
        fetch_k(0).wait()
        fetch_k(2).start()
    with jax.named_scope("weigh"):
        for g in range(groups):
            wbuf[g] = softmaxed(scored(0, g))
    with jax.named_scope("wait_wo"):
        for cp in second:
            cp.wait()
    with jax.named_scope("barrier_wait"):
        pl.semaphore_wait(barrier, n - 1)

    def attend(c, _):
        with jax.named_scope("k_wait"):
            fetch_k(c).wait()
        with jax.named_scope("v_wait"):
            fetch_v(c - 1).wait()

        @pl.when(c + 1 < chunks)
        def _():
            fetch_v(c + 1).start()

        @pl.when(c + 2 < chunks)
        def _():
            fetch_k(c + 2).start()

        @pl.when(c + 2 == chunks)
        def _():
            third[0].start()

        @pl.when(c + 1 == chunks)
        def _():
            third[1].start()

        with jax.named_scope("attend"):
            before = [wbuf[g] for g in range(groups)]
            scores = [scored(c, g) for g in range(groups)]
            o = [mixed(c - 1, g, before[g]) for g in range(groups)]
            for g in range(groups):
                wbuf[g] = softmaxed(scores[g])
            project(c - 1, o)
        with jax.named_scope("send"):
            send(c - 1)

        @pl.when(c - 1 >= LAG)
        def _():
            finish(c - 1 - LAG)

        return 0

    lax.fori_loop(1, chunks, attend, 0)
    with jax.named_scope("v_wait"):
        fetch_v(chunks - 1).wait()
    third[2].start()
    with jax.named_scope("mix"):
        project(chunks - 1, [mixed(chunks - 1, g, wbuf[g]) for g in range(groups)])
    with jax.named_scope("send"):
        send(chunks - 1)
    for c in range(chunks - 1 - LAG, chunks - 1):
        finish(c)

    gmv = gm[...].astype(F32)

    def rs2_copy(p, j):
        return pltpu.make_async_remote_copy(
            src_ref=passes[4 * p + 1].at[peer(j)], dst_ref=passes[4 * p + 2].at[j - 1], send_sem=rs2_s.at[p],
            recv_sem=rs2_r.at[p], device_id={"tp": peer(j)})

    def ag2_copy(p, j):
        ybuf = passes[4 * p + 3]
        return pltpu.make_async_remote_copy(
            src_ref=ybuf.at[me], dst_ref=ybuf.at[me], send_sem=ag2_s.at[p], recv_sem=ag2_r.at[p],
            device_id={"tp": peer(j)})

    def feed(p, lo, hi, between=None):
        p2, s2 = passes[4 * p:4 * p + 2]
        count = (hi - lo) * CH
        with jax.named_scope("ag_wait"):
            for c in range(lo, hi):
                all_of(rbuf.at[c], ag_r.at[c])

        def h_block(j):
            return hbuf[lo:hi, j].astype(F32).reshape(count, blk)

        with jax.named_scope("feed"):
            total = None
            for j in range(n):
                hj = h_block(j)
                t = jnp.sum(hj * hj, -1, keepdims=True)
                total = t if total is None else total + t
            scale = lax.rsqrt(total * (1.0 / d) + 1e-6)
            at_rows = slice(lo * CH, hi * CH)
            for j in range(n):
                hj = h_block(j)
                for i in range(blk // 128):
                    g = j * (blk // 128) + i
                    bbuf[at_rows, 128 * g:128 * g + 128] = (hj[:, 128 * i:128 * i + 128] * scale * gmv[g:g + 1]).astype(BF16)
        if p == 0:
            with jax.named_scope("w_wait"):
                for cp in third:
                    cp.wait()
        with jax.named_scope("mlp"):
            hidden = []
            for f in range(wg.shape[1] // 256):
                at = slice(256 * f, 256 * f + 256)
                gate = dot(bbuf[at_rows, :], wg[:, at])
                up = dot(bbuf[at_rows, :], wu[:, at])
                hidden.append((jax.nn.silu(gate) * up).astype(BF16))
            hidden = jnp.concatenate(hidden, 1)
        if between is not None:
            between()
        with jax.named_scope("down"):
            for j in range(n):
                part = dot(hidden, wd[:, blk * j:blk * (j + 1)])
                p2[j] = part
                s2[j] = part.astype(BF16)
        with jax.named_scope("send2"):
            for j in far_first:
                rs2_copy(p, j).start()

    def finish2(p, lo, hi):
        p2, _, r2, ybuf = passes[4 * p:4 * p + 4]
        with jax.named_scope("rs2_wait"):
            all_of(r2, rs2_r.at[p])
        with jax.named_scope("sum2"):
            total = p2[me]
            for j in range(n - 1):
                total = total + r2[j].astype(F32)
            total = total + hbuf[lo:hi, me].astype(F32).reshape((hi - lo) * CH, blk)
            ybuf[me] = total.astype(BF16)
            for j in far_first:
                ag2_copy(p, j).start()

    def close(p, lo, hi):
        _, _, r2, ybuf = passes[4 * p:4 * p + 4]
        with jax.named_scope("ag2_wait"):
            all_of(r2, ag2_r.at[p])
        with jax.named_scope("out"):
            for j in range(n):
                y_ref[lo * CH:hi * CH, blk * j:blk * (j + 1)] = ybuf[j]

    ends = [sum(PASSES[:p + 1]) for p in range(len(PASSES))]
    parts = [(hi - count, hi) for hi, count in zip(ends, PASSES)]
    for p, (lo, hi) in enumerate(parts):
        feed(p, lo, hi, functools.partial(finish, chunks - 1) if p == 0 else None)
    for p, (lo, hi) in enumerate(parts):
        finish2(p, lo, hi)
    with jax.named_scope("sends_wait"):
        for c in range(chunks):
            all_of(rbuf.at[c], rs_s.at[c])
            all_of(rbuf.at[c], ag_s.at[c])
    for p, (lo, hi) in enumerate(parts):
        close(p, lo, hi)
    for p in range(len(PASSES)):
        r2 = passes[4 * p + 2]
        all_of(r2, rs2_s.at[p])
        all_of(r2, ag2_s.at[p])


def solution(mesh):
    n = mesh.shape["tp"]

    def step(x, k_cache, v_cache, gain_a, wq, wo, gain_m, w_gate, w_up, w_down):
        rows, d = x.shape
        batch, cache, heads, head = k_cache.shape
        ff = w_gate.shape[1]
        chunks, blk = rows // CH, d // n
        half = head // 2
        angle = (cache - 1) * float(THETA) ** (-np.arange(half) / half)
        cos, sin = np.cos(angle), np.sin(angle)
        cs = np.zeros((8, head), np.float32)
        cs[0], cs[1] = np.concatenate([cos, cos]), np.concatenate([-sin, sin])
        keys = k_cache.reshape(batch, cache * heads, head)
        values = v_cache.reshape(batch, cache * heads, head)
        second_half = []
        assert sum(PASSES) == chunks
        for count in (CH * p for p in PASSES):
            second_half += [
                pltpu.VMEM((n, count, blk), F32),
                pltpu.VMEM((n, count, blk), BF16),
                pltpu.VMEM((n - 1, count, blk), BF16),
                pltpu.VMEM((n, count, blk), BF16),
            ]
        dma = pltpu.SemaphoreType.DMA
        return pl.pallas_call(
            functools.partial(kernel, n),
            out_shape=jax.ShapeDtypeStruct((rows, d), BF16),
            in_specs=[pl.BlockSpec(memory_space=pl.ANY)] * 11,
            out_specs=pl.BlockSpec(memory_space=pltpu.VMEM),
            scratch_shapes=[
                pltpu.VMEM((rows, d), BF16),
                pltpu.VMEM((rows, d), F32),
                pltpu.VMEM((d // 128, 128), BF16),
                pltpu.VMEM((d // 128, 128), BF16),
                pltpu.VMEM((8, head), F32),
                pltpu.VMEM(wq.shape, BF16),
                pltpu.VMEM(wo.shape, BF16),
                pltpu.VMEM(w_gate.shape, BF16),
                pltpu.VMEM(w_up.shape, BF16),
                pltpu.VMEM(w_down.shape, BF16),
                pltpu.VMEM((SLOTS, CH, cache * heads, head), BF16),
                pltpu.VMEM((SLOTS, CH, cache * heads, head), BF16),
                pltpu.VMEM((rows // GROUP, heads * GROUP, head), F32),
                pltpu.VMEM((CH // GROUP, 4 * GROUP, cache * heads // 2), F32),
                pltpu.VMEM((chunks, n, CH, blk), F32),
                pltpu.VMEM((chunks, n, CH, blk), BF16),
                pltpu.VMEM((chunks, n - 1, CH, blk), BF16),
                pltpu.VMEM((chunks, n, CH, blk), BF16),
                pltpu.VMEM((rows, d), BF16),
                *second_half,
                dma((9,)), dma((SLOTS,)), dma((SLOTS,)),
                dma((chunks,)), dma((chunks,)), dma((chunks,)), dma((chunks,)),
                *[dma((len(PASSES),))] * 4,
            ],
            compiler_params=pltpu.CompilerParams(
                collective_id=0, has_side_effects=True, vmem_limit_bytes=64 * 1024 * 1024 - 65536),
            name="decoder_layer",
        )(x, keys, values, gain_a.reshape(d // 128, 128), wq, wo, gain_m.reshape(d // 128, 128), w_gate, w_up, w_down, jnp.asarray(cs))

    states, cache, columns, rows_of = P("dp", None), P("dp", None, "tp", None), P(None, "tp"), P("tp", None)
    return jax.shard_map(
        step,
        mesh=mesh,
        in_specs=(states, cache, cache, P(None), columns, rows_of, P(None), columns, columns, rows_of),
        out_specs=states,
        check_vma=False,
    )
```

```python
import functools

import jax
import jax.numpy as jnp
import numpy as np
from jax import lax
from jax.experimental import pallas as pl
from jax.experimental.pallas import tpu as pltpu
from jax.sharding import PartitionSpec as P

HEAD = 128
THETA = 10000
F32, BF16 = jnp.float32, jnp.bfloat16

CH = 8
SLOTS = 3
AHEAD = 2
LAG = 2
GROUP = 4
PASSES = (2, 2, 2, 2)


def dot(a, b):
    return lax.dot_general(a, b, (((1,), (0,)), ((), ())), preferred_element_type=F32)


def dot_t(a, b):
    return lax.dot_general(a, b, (((1,), (1,)), ((), ())), preferred_element_type=F32)


def kernel(n, x_hbm, k_hbm, v_hbm, ga_hbm, wq_hbm, wo_hbm, gm_hbm, wg_hbm, wu_hbm, wd_hbm, cs_hbm, y_ref,
           xb, xf, ga, gm, cs, wq, wo, wg, wu, wd, kbuf, vbuf, qf, wbuf, pf, sbuf, rbuf, hbuf, bbuf, *rest):
    passes, (sem_in, sem_k, sem_v, rs_s, rs_r, ag_s, ag_r, rs2_s, rs2_r, ag2_s, ag2_r) = rest[:-11], rest[-11:]
    me = lax.axis_index("tp")
    rows, d = xb.shape
    chunks = rows // CH
    blk = d // n
    span = kbuf.shape[2] // 2

    far_first = sorted(range(1, n), key=lambda j: -min(j, n - j))

    def peer(j):
        return lax.rem(me + j, n)

    def load(i, src, dst):
        return pltpu.make_async_copy(src, dst, sem_in.at[i])

    first = [load(0, x_hbm, xb), load(1, ga_hbm, ga), load(2, cs_hbm, cs), load(3, wq_hbm, wq)]
    second = [load(4, wo_hbm, wo), load(5, gm_hbm, gm)]

    def load_part(i, src, dst, part):
        at = pl.ds(part * (src.shape[0] // 2), src.shape[0] // 2)
        return pltpu.make_async_copy(src.at[at], dst.at[at], sem_in.at[i])

    third = [load_part(6 + 2 * i + part, src, dst, part)
             for i, (src, dst) in enumerate(((wg_hbm, wg), (wu_hbm, wu), (wd_hbm, wd))) for part in range(2)]

    class Fetch:
        def __init__(self, hbm, buf, sem, c):
            self.hbm, self.c, slot = hbm, c, lax.rem(c, SLOTS)
            self.buf, self.sem = buf.at[slot], sem.at[slot]

        def start(self):
            for g in range(0, CH, GROUP):
                pltpu.make_async_copy(self.hbm.at[pl.ds(self.c * CH + g, GROUP)], self.buf.at[pl.ds(g, GROUP)], self.sem).start()

        def wait(self):
            pltpu.make_async_copy(self.hbm.at[pl.ds(self.c * CH, CH)], self.buf, self.sem).wait()

    def fetch_k(c):
        return Fetch(k_hbm, kbuf, sem_k, c)

    def fetch_v(c):
        return Fetch(v_hbm, vbuf, sem_v, c)

    with jax.named_scope("start"):
        for cp in first:
            cp.start()
        fetch_k(0).start()
        barrier = pltpu.get_barrier_semaphore()
        for j in range(1, n):
            pl.semaphore_signal(barrier, inc=1, device_id={"tp": peer(j)})

    with jax.named_scope("wait_x"):
        for cp in first[:3]:
            cp.wait()
    with jax.named_scope("norm"):
        fetch_k(1).start()
        fetch_v(0).start()
        xv = xb[...].astype(F32)
        xf[...] = xv
        scale = lax.rsqrt(jnp.sum(xv * xv, -1, keepdims=True) * (1.0 / d) + 1e-6)
        gav = ga[...].astype(F32)
        for i in range(d // 128):
            at = slice(128 * i, 128 * i + 128)
            bbuf[:, at] = (xf[:, at] * scale * gav[i:i + 1]).astype(BF16)
    with jax.named_scope("wait_wq"):
        first[3].wait()
        for cp in second:
            cp.start()
        fetch_k(2).start()
    with jax.named_scope("qproj"):
        q = dot(bbuf[...], wq[...]).astype(BF16).astype(F32)
        for g in range(2):
            t = q[:, HEAD * g:HEAD * (g + 1)]
            turned = (t * cs[0:1] + pltpu.roll(t, HEAD // 2, 1) * cs[1:2]).astype(BF16).astype(F32)
            for i in range(rows // GROUP):
                qf[i, GROUP * g:GROUP * (g + 1)] = turned[GROUP * i:GROUP * (i + 1)]

    def rs_copy(c, j):
        return pltpu.make_async_remote_copy(
            src_ref=sbuf.at[c, peer(j)], dst_ref=rbuf.at[c, j - 1], send_sem=rs_s.at[c], recv_sem=rs_r.at[c],
            device_id={"tp": peer(j)})

    def ag_copy(c, j):
        return pltpu.make_async_remote_copy(
            src_ref=hbuf.at[c, me], dst_ref=hbuf.at[c, me], send_sem=ag_s.at[c], recv_sem=ag_r.at[c],
            device_id={"tp": peer(j)})

    def all_of(ref, sem):
        pltpu.make_async_copy(ref, ref, sem).wait()

    def finish(c):
        with jax.named_scope("finish_wait"):
            all_of(rbuf.at[c], rs_r.at[c])
        with jax.named_scope("finish"):
            total = pf[c, me]
            for j in range(n - 1):
                total = total + rbuf[c, j].astype(F32)
            total = total + xf[pl.ds(pl.multiple_of(c * CH, CH), CH), pl.ds(pl.multiple_of(me * blk, blk), blk)]
            hbuf[c, me] = total.astype(BF16)
            for j in far_first:
                ag_copy(c, j).start()

    tall = 4 * GROUP
    row = lax.broadcasted_iota(jnp.int32, (tall, 2 * HEAD), 0)
    row_w = lax.broadcasted_iota(jnp.int32, (tall, span), 0)
    col_w = lax.broadcasted_iota(jnp.int32, (tall, span), 1)
    own_head = (col_w % 2) == ((row_w // GROUP) % 2)
    groups = CH // GROUP

    def scored(c, g):
        slot = lax.rem(c, SLOTS)
        qg = qf[c * groups + g]
        zero = jnp.zeros_like(qg)
        base = jnp.concatenate([jnp.concatenate([qg, zero], 1), jnp.concatenate([zero, qg], 1)], 0)
        s = None
        for i in range(GROUP):
            lhs = jnp.where(row % GROUP == i, base, 0.0).astype(BF16)
            at = g * GROUP + i
            t = dot_t(lhs, jnp.concatenate([kbuf[slot, at, :span], kbuf[slot, at, span:]], 1))
            s = t if s is None else s + t
        return s

    def softmaxed(s):
        half = tall // 2
        s = jnp.where(own_head, s * HEAD**-0.5, -jnp.inf)
        m = jnp.max(s, -1, keepdims=True)
        m = jnp.maximum(m[:half], m[half:])
        e = jnp.exp(s - jnp.concatenate([m, m], 0))
        z = jnp.sum(e, -1, keepdims=True)
        z = 1.0 / (z[:half] + z[half:])
        return e * jnp.concatenate([z, z], 0)

    def mixed(c, g, w):
        slot = lax.rem(c, SLOTS)
        o = None
        for i in range(GROUP):
            lhs = jnp.where(row_w % GROUP == i, w, 0.0).astype(BF16)
            at = g * GROUP + i
            t = dot(lhs, jnp.concatenate([vbuf[slot, at, :span], vbuf[slot, at, span:]], 1))
            o = t if o is None else o + t
        return o[:tall // 2, :HEAD] + o[tall // 2:, HEAD:]

    def project(c, o):
        upper = lax.broadcasted_iota(jnp.int32, (CH, HEAD), 0) < GROUP
        head0 = jnp.where(upper, o[0], pltpu.roll(o[1], GROUP, 0))
        head1 = jnp.where(upper, pltpu.roll(o[0], GROUP, 0), o[1])
        seen = jnp.concatenate([head0, head1], 1).astype(BF16)
        term = dot(seen, wo[...])
        for j in range(n):
            part = term[:, blk * j:blk * (j + 1)]
            pf[c, j] = part
            sbuf[c, j] = part.astype(BF16)

    def send(c):
        for j in far_first:
            rs_copy(c, j).start()

    for c in range(AHEAD):
        with jax.named_scope("k_wait"):
            fetch_k(c).wait()
        with jax.named_scope("weigh"):
            for g in range(groups):
                wbuf[c, g] = softmaxed(scored(c, g))
        if c + 1 < AHEAD:
            fetch_v(c + 1).start()
            fetch_k(c + SLOTS).start()
    with jax.named_scope("wait_wo"):
        for cp in second:
            cp.wait()
    with jax.named_scope("barrier_wait"):
        pl.semaphore_wait(barrier, n - 1)

    def attend(c, _):
        ready = c - AHEAD
        with jax.named_scope("k_wait"):
            fetch_k(c).wait()
        with jax.named_scope("v_wait"):
            fetch_v(ready).wait()
        fetch_v(c).start()

        @pl.when(c + 2 < chunks)
        def _():
            fetch_k(c + 2).start()

        @pl.when(c + 1 == chunks)
        def _():
            third[0].start()

        with jax.named_scope("attend"):
            at = lax.rem(c, AHEAD)
            before = [wbuf[at, g] for g in range(groups)]
            scores = [scored(c, g) for g in range(groups)]
            o = [mixed(ready, g, before[g]) for g in range(groups)]
            for g in range(groups):
                wbuf[at, g] = softmaxed(scores[g])
            project(ready, o)
        with jax.named_scope("send"):
            send(ready)

        @pl.when(ready >= LAG)
        def _():
            finish(ready - LAG)

        return 0

    lax.fori_loop(AHEAD, chunks, attend, 0)
    for cp in third[1:]:
        cp.start()
    rest_of = range(chunks - AHEAD, chunks)
    with jax.named_scope("v_wait"):
        for c in rest_of:
            fetch_v(c).wait()
    with jax.named_scope("mix"):
        o = [[mixed(c, g, wbuf[c % AHEAD, g]) for g in range(groups)] for c in rest_of]
        for c in rest_of:
            project(c, o[c - rest_of[0]])
    with jax.named_scope("send"):
        for c in rest_of:
            send(c)
    finish(chunks - 4)

    ends = [sum(PASSES[:p + 1]) for p in range(len(PASSES))]
    parts = [(hi - count, hi) for hi, count in zip(ends, PASSES)]
    gmv = gm[...].astype(F32)

    def rs2_copy(p, j):
        return pltpu.make_async_remote_copy(
            src_ref=passes[4 * p + 1].at[peer(j)], dst_ref=passes[4 * p + 2].at[j - 1], send_sem=rs2_s.at[p],
            recv_sem=rs2_r.at[p], device_id={"tp": peer(j)})

    def own_part(p):
        lo, hi = parts[p]
        return y_ref.at[pl.ds(lo * CH, (hi - lo) * CH), pl.ds(pl.multiple_of(me * blk, blk), blk)]

    def ag2_copy(p, j):
        return pltpu.make_async_remote_copy(
            src_ref=passes[4 * p + 3], dst_ref=own_part(p), send_sem=ag2_s.at[p], recv_sem=ag2_r.at[p],
            device_id={"tp": peer(j)})

    def feed(p, lo, hi, between=None):
        p2, s2 = passes[4 * p:4 * p + 2]
        count = (hi - lo) * CH
        with jax.named_scope("ag_wait"):
            for c in range(lo, hi):
                all_of(rbuf.at[c], ag_r.at[c])

        def h_block(j):
            return hbuf[lo:hi, j].astype(F32).reshape(count, blk)

        with jax.named_scope("feed"):
            total = None
            for j in range(n):
                hj = h_block(j)
                t = jnp.sum(hj * hj, -1, keepdims=True)
                total = t if total is None else total + t
            scale = lax.rsqrt(total * (1.0 / d) + 1e-6)
            at_rows = slice(lo * CH, hi * CH)
            for j in range(n):
                hj = h_block(j)
                for i in range(blk // 128):
                    g = j * (blk // 128) + i
                    bbuf[at_rows, 128 * g:128 * g + 128] = (hj[:, 128 * i:128 * i + 128] * scale * gmv[g:g + 1]).astype(BF16)
        if p == 0:
            with jax.named_scope("w_wait"):
                for cp in third[:4]:
                    cp.wait()
        with jax.named_scope("mlp"):
            hidden = []
            for f in range(wg.shape[1] // 256):
                at = slice(256 * f, 256 * f + 256)
                gate = dot(bbuf[at_rows, :], wg[:, at])
                up = dot(bbuf[at_rows, :], wu[:, at])
                hidden.append((jax.nn.silu(gate) * up).astype(BF16))
            hidden = jnp.concatenate(hidden, 1)
        if between is not None:
            finish(between)
        if p == 0:
            with jax.named_scope("w_wait"):
                for cp in third[4:]:
                    cp.wait()
        with jax.named_scope("down"):
            for j in range(n):
                part = dot(hidden, wd[:, blk * j:blk * (j + 1)])
                p2[j] = part
                s2[j] = part.astype(BF16)
        with jax.named_scope("send2"):
            for j in far_first:
                rs2_copy(p, j).start()

    def finish2(p, lo, hi):
        p2, _, r2, ybuf = passes[4 * p:4 * p + 4]
        with jax.named_scope("rs2_wait"):
            all_of(r2, rs2_r.at[p])
        with jax.named_scope("sum2"):
            total = p2[me]
            for j in range(n - 1):
                total = total + r2[j].astype(F32)
            total = total + hbuf[lo:hi, me].astype(F32).reshape((hi - lo) * CH, blk)
            ybuf[...] = total.astype(BF16)
            own_part(p)[...] = ybuf[...]
            for j in far_first:
                ag2_copy(p, j).start()

    last = len(parts) - 1
    for p, (lo, hi) in enumerate(parts):
        if p == last:
            finish2(0, *parts[0])
        feed(p, lo, hi, chunks - 3 if p == 0 else None)
        if p == 0:
            finish(chunks - 2)
            finish(chunks - 1)
    for p, (lo, hi) in enumerate(parts[1:], 1):
        finish2(p, lo, hi)
    with jax.named_scope("sends_wait"):
        for c in range(chunks):
            all_of(rbuf.at[c], rs_s.at[c])
            all_of(rbuf.at[c], ag_s.at[c])
    for p in range(len(PASSES)):
        r2 = passes[4 * p + 2]
        all_of(r2, rs2_s.at[p])
        all_of(r2, ag2_s.at[p])
        with jax.named_scope("ag2_wait"):
            all_of(r2, ag2_r.at[p])


def put_out(y_ref, out_ref, sem):
    copy = pltpu.make_async_copy(y_ref, out_ref, sem)
    copy.start()
    copy.wait()


def solution(mesh):
    n = mesh.shape["tp"]

    def step(x, k_cache, v_cache, gain_a, wq, wo, gain_m, w_gate, w_up, w_down):
        rows, d = x.shape
        batch, cache, heads, head = k_cache.shape
        ff = w_gate.shape[1]
        chunks, blk = rows // CH, d // n
        half = head // 2
        angle = (cache - 1) * float(THETA) ** (-np.arange(half) / half)
        cos, sin = np.cos(angle), np.sin(angle)
        cs = np.zeros((8, head), np.float32)
        cs[0], cs[1] = np.concatenate([cos, cos]), np.concatenate([-sin, sin])
        keys = k_cache.reshape(batch, cache * heads, head)
        values = v_cache.reshape(batch, cache * heads, head)
        second_half = []
        assert sum(PASSES) == chunks
        for count in (CH * p for p in PASSES):
            second_half += [
                pltpu.VMEM((n, count, blk), F32),
                pltpu.VMEM((n, count, blk), BF16),
                pltpu.VMEM((n - 1, count, blk), BF16),
                pltpu.VMEM((count, blk), BF16),
            ]
        dma = pltpu.SemaphoreType.DMA
        y = pl.pallas_call(
            functools.partial(kernel, n),
            out_shape=pltpu.VMEM((rows, d), BF16),
            in_specs=[pl.BlockSpec(memory_space=pl.ANY)] * 11,
            out_specs=pl.BlockSpec(memory_space=pltpu.VMEM),
            scratch_shapes=[
                pltpu.VMEM((rows, d), BF16),
                pltpu.VMEM((rows, d), F32),
                pltpu.VMEM((d // 128, 128), BF16),
                pltpu.VMEM((d // 128, 128), BF16),
                pltpu.VMEM((8, head), F32),
                pltpu.VMEM(wq.shape, BF16),
                pltpu.VMEM(wo.shape, BF16),
                pltpu.VMEM(w_gate.shape, BF16),
                pltpu.VMEM(w_up.shape, BF16),
                pltpu.VMEM(w_down.shape, BF16),
                pltpu.VMEM((SLOTS, CH, cache * heads, head), BF16),
                pltpu.VMEM((SLOTS, CH, cache * heads, head), BF16),
                pltpu.VMEM((rows // GROUP, heads * GROUP, head), F32),
                pltpu.VMEM((AHEAD, CH // GROUP, 4 * GROUP, cache * heads // 2), F32),
                pltpu.VMEM((chunks, n, CH, blk), F32),
                pltpu.VMEM((chunks, n, CH, blk), BF16),
                pltpu.VMEM((chunks, n - 1, CH, blk), BF16),
                pltpu.VMEM((chunks, n, CH, blk), BF16),
                pltpu.VMEM((rows, d), BF16),
                *second_half,
                dma((12,)), dma((SLOTS,)), dma((SLOTS,)),
                dma((chunks,)), dma((chunks,)), dma((chunks,)), dma((chunks,)),
                *[dma((len(PASSES),))] * 4,
            ],
            compiler_params=pltpu.CompilerParams(
                collective_id=0, has_side_effects=True, vmem_limit_bytes=64336 * 1024),
            name="decoder_layer",
        )(x, keys, values, gain_a.reshape(d // 128, 128), wq, wo, gain_m.reshape(d // 128, 128), w_gate, w_up, w_down, jnp.asarray(cs))
        return pl.pallas_call(
            put_out,
            out_shape=jax.ShapeDtypeStruct((rows, d), BF16),
            in_specs=[pl.BlockSpec(memory_space=pltpu.VMEM)],
            out_specs=pl.BlockSpec(memory_space=pl.ANY),
            scratch_shapes=[dma(())],
            compiler_params=pltpu.CompilerParams(vmem_limit_bytes=1024 * 1024),
            name="put_out",
        )(y)

    states, cache, columns, rows_of = P("dp", None), P("dp", None, "tp", None), P(None, "tp"), P("tp", None)
    return jax.shard_map(
        step,
        mesh=mesh,
        in_specs=(states, cache, cache, P(None), columns, rows_of, P(None), columns, columns, rows_of),
        out_specs=states,
        check_vma=False,
    )
```

```python
import functools

import jax
import jax.numpy as jnp
import numpy as np
from jax import lax
from jax.experimental import pallas as pl
from jax.experimental.pallas import tpu as pltpu
from jax.sharding import PartitionSpec as P

HEAD = 128
THETA = 10000
F32, BF16 = jnp.float32, jnp.bfloat16

CH = 8
SLOTS = 3
AHEAD = 1
LAG = 2
GROUP = 4
PASSES = (4, 2, 2)


def dot(a, b):
    return lax.dot_general(a, b, (((1,), (0,)), ((), ())), preferred_element_type=F32)


def dot_t(a, b):
    return lax.dot_general(a, b, (((1,), (1,)), ((), ())), preferred_element_type=F32)


def kernel(n, x_hbm, k_hbm, v_hbm, ga_hbm, wq_hbm, wo_hbm, gm_hbm, wg_hbm, wu_hbm, wd_hbm, cs_hbm, y_ref,
           xb, xf, ga, gm, cs, wq, wo, wg, wu, wd, kbuf, vbuf, qf, wbuf, pf, sbuf, rbuf, hbuf, bbuf, *rest):
    passes, (sem_in, sem_k, sem_v, rs_s, rs_r, ag_s, ag_r, rs2_s, rs2_r, ag2_s, ag2_r) = rest[:-11], rest[-11:]
    me = lax.axis_index("tp")
    rows, d = xb.shape
    chunks = rows // CH
    blk = d // n
    span = kbuf.shape[2] // 2

    far_first = sorted(range(1, n), key=lambda j: -min(j, n - j))

    def peer(j):
        return lax.rem(me + j, n)

    def load(i, src, dst):
        return pltpu.make_async_copy(src, dst, sem_in.at[i])

    first = [load(0, x_hbm, xb), load(1, ga_hbm, ga), load(2, cs_hbm, cs), load(3, wq_hbm, wq)]
    second = [load(4, wo_hbm, wo), load(5, gm_hbm, gm)]

    def load_part(i, src, dst, part):
        at = pl.ds(part * (src.shape[0] // 2), src.shape[0] // 2)
        return pltpu.make_async_copy(src.at[at], dst.at[at], sem_in.at[i])

    third = [load_part(6 + 2 * i + part, src, dst, part)
             for i, (src, dst) in enumerate(((wg_hbm, wg), (wu_hbm, wu), (wd_hbm, wd))) for part in range(2)]

    class Fetch:
        def __init__(self, hbm, buf, sem, c):
            self.hbm, self.c, slot = hbm, c, lax.rem(c, SLOTS)
            self.buf, self.sem = buf.at[slot], sem.at[slot]

        def start(self):
            for g in range(0, CH, GROUP):
                pltpu.make_async_copy(self.hbm.at[pl.ds(self.c * CH + g, GROUP)], self.buf.at[pl.ds(g, GROUP)], self.sem).start()

        def wait(self):
            pltpu.make_async_copy(self.hbm.at[pl.ds(self.c * CH, CH)], self.buf, self.sem).wait()

    def fetch_k(c):
        return Fetch(k_hbm, kbuf, sem_k, c)

    def fetch_v(c):
        return Fetch(v_hbm, vbuf, sem_v, c)

    with jax.named_scope("start"):
        for cp in first:
            cp.start()
        fetch_k(0).start()
        barrier = pltpu.get_barrier_semaphore()
        for j in range(1, n):
            pl.semaphore_signal(barrier, inc=1, device_id={"tp": peer(j)})

    with jax.named_scope("wait_x"):
        for cp in first[:3]:
            cp.wait()
    with jax.named_scope("norm"):
        fetch_v(0).start()
        fetch_k(1).start()
        xv = xb[...].astype(F32)
        xf[...] = xv
        scale = lax.rsqrt(jnp.sum(xv * xv, -1, keepdims=True) * (1.0 / d) + 1e-6)
        gav = ga[...].astype(F32)
        for i in range(d // 128):
            at = slice(128 * i, 128 * i + 128)
            bbuf[:, at] = (xf[:, at] * scale * gav[i:i + 1]).astype(BF16)
    with jax.named_scope("wait_wq"):
        first[3].wait()
        for cp in second:
            cp.start()
        fetch_v(1).start()
    with jax.named_scope("qproj"):
        q = dot(bbuf[...], wq[...]).astype(BF16).astype(F32)
        for g in range(2):
            t = q[:, HEAD * g:HEAD * (g + 1)]
            turned = (t * cs[0:1] + pltpu.roll(t, HEAD // 2, 1) * cs[1:2]).astype(BF16).astype(F32)
            for i in range(rows // GROUP):
                qf[i, GROUP * g:GROUP * (g + 1)] = turned[GROUP * i:GROUP * (i + 1)]

    def rs_copy(c, j):
        return pltpu.make_async_remote_copy(
            src_ref=sbuf.at[c, peer(j)], dst_ref=rbuf.at[c, j - 1], send_sem=rs_s.at[c], recv_sem=rs_r.at[c],
            device_id={"tp": peer(j)})

    def ag_copy(c, j):
        return pltpu.make_async_remote_copy(
            src_ref=hbuf.at[c, me], dst_ref=hbuf.at[c, me], send_sem=ag_s.at[c], recv_sem=ag_r.at[c],
            device_id={"tp": peer(j)})

    def all_of(ref, sem):
        pltpu.make_async_copy(ref, ref, sem).wait()

    def finish(c):
        with jax.named_scope("finish_wait"):
            all_of(rbuf.at[c], rs_r.at[c])
        with jax.named_scope("finish"):
            total = pf[c, me]
            for j in range(n - 1):
                total = total + rbuf[c, j].astype(F32)
            total = total + xf[pl.ds(pl.multiple_of(c * CH, CH), CH), pl.ds(pl.multiple_of(me * blk, blk), blk)]
            hbuf[c, me] = total.astype(BF16)
            for j in far_first:
                ag_copy(c, j).start()

    tall = 4 * GROUP
    row = lax.broadcasted_iota(jnp.int32, (tall, 2 * HEAD), 0)
    row_w = lax.broadcasted_iota(jnp.int32, (tall, span), 0)
    col_w = lax.broadcasted_iota(jnp.int32, (tall, span), 1)
    own_head = (col_w % 2) == ((row_w // GROUP) % 2)
    groups = CH // GROUP

    def scored(c, g):
        slot = lax.rem(c, SLOTS)
        qg = qf[c * groups + g]
        zero = jnp.zeros_like(qg)
        base = jnp.concatenate([jnp.concatenate([qg, zero], 1), jnp.concatenate([zero, qg], 1)], 0)
        s = None
        for i in range(GROUP):
            lhs = jnp.where(row % GROUP == i, base, 0.0).astype(BF16)
            at = g * GROUP + i
            t = dot_t(lhs, jnp.concatenate([kbuf[slot, at, :span], kbuf[slot, at, span:]], 1))
            s = t if s is None else s + t
        return s

    def softmaxed(s):
        half = tall // 2
        s = jnp.where(own_head, s * HEAD**-0.5, -jnp.inf)
        m = jnp.max(s, -1, keepdims=True)
        m = jnp.maximum(m[:half], m[half:])
        e = jnp.exp(s - jnp.concatenate([m, m], 0))
        z = jnp.sum(e, -1, keepdims=True)
        z = 1.0 / (z[:half] + z[half:])
        return e * jnp.concatenate([z, z], 0)

    def mixed(c, g, w):
        slot = lax.rem(c, SLOTS)
        o = None
        for i in range(GROUP):
            lhs = jnp.where(row_w % GROUP == i, w, 0.0).astype(BF16)
            at = g * GROUP + i
            t = dot(lhs, jnp.concatenate([vbuf[slot, at, :span], vbuf[slot, at, span:]], 1))
            o = t if o is None else o + t
        return o[:tall // 2, :HEAD] + o[tall // 2:, HEAD:]

    def project(c, o):
        upper = lax.broadcasted_iota(jnp.int32, (CH, HEAD), 0) < GROUP
        head0 = jnp.where(upper, o[0], pltpu.roll(o[1], GROUP, 0))
        head1 = jnp.where(upper, pltpu.roll(o[0], GROUP, 0), o[1])
        seen = jnp.concatenate([head0, head1], 1).astype(BF16)
        term = dot(seen, wo[...])
        for j in range(n):
            part = term[:, blk * j:blk * (j + 1)]
            pf[c, j] = part
            sbuf[c, j] = part.astype(BF16)

    def send(c):
        for j in far_first:
            rs_copy(c, j).start()

    with jax.named_scope("k_wait"):
        fetch_k(0).wait()
        fetch_k(2).start()
    with jax.named_scope("weigh"):
        for g in range(groups):
            wbuf[0, g] = softmaxed(scored(0, g))
    with jax.named_scope("wait_wo"):
        for cp in second:
            cp.wait()
    with jax.named_scope("barrier_wait"):
        pl.semaphore_wait(barrier, n - 1)

    def attend(c, _):
        ready = c - AHEAD
        with jax.named_scope("k_wait"):
            fetch_k(c).wait()
        with jax.named_scope("v_wait"):
            fetch_v(ready).wait()

        @pl.when(c + 1 < chunks)
        def _():
            fetch_v(c + 1).start()

        @pl.when(c + 2 < chunks)
        def _():
            fetch_k(c + 2).start()

        @pl.when(c + 1 == chunks)
        def _():
            for cp in third[:4]:
                cp.start()

        with jax.named_scope("attend"):
            at = lax.rem(c, AHEAD)
            before = [wbuf[at, g] for g in range(groups)]
            scores = [scored(c, g) for g in range(groups)]
            o = [mixed(ready, g, before[g]) for g in range(groups)]
            for g in range(groups):
                wbuf[at, g] = softmaxed(scores[g])
            project(ready, o)
        with jax.named_scope("send"):
            send(ready)

        @pl.when(ready >= LAG)
        def _():
            finish(ready - LAG)

        return 0

    lax.fori_loop(AHEAD, chunks, attend, 0)
    rest_of = range(chunks - AHEAD, chunks)
    with jax.named_scope("v_wait"):
        for c in rest_of:
            fetch_v(c).wait()
        for cp in third[4:]:
            cp.start()
    with jax.named_scope("mix"):
        o = [[mixed(c, g, wbuf[c % AHEAD, g]) for g in range(groups)] for c in rest_of]
        for c in rest_of:
            project(c, o[c - rest_of[0]])
    with jax.named_scope("send"):
        for c in rest_of:
            send(c)
    finish(chunks - 3)

    ends = [sum(PASSES[:p + 1]) for p in range(len(PASSES))]
    parts = [(hi - count, hi) for hi, count in zip(ends, PASSES)]
    gmv = gm[...].astype(F32)

    def rs2_copy(p, j):
        return pltpu.make_async_remote_copy(
            src_ref=passes[4 * p + 1].at[peer(j)], dst_ref=passes[4 * p + 2].at[j - 1], send_sem=rs2_s.at[p],
            recv_sem=rs2_r.at[p], device_id={"tp": peer(j)})

    def own_part(p):
        lo, hi = parts[p]
        return y_ref.at[pl.ds(lo * CH, (hi - lo) * CH), pl.ds(pl.multiple_of(me * blk, blk), blk)]

    def ag2_copy(p, j):
        return pltpu.make_async_remote_copy(
            src_ref=passes[4 * p + 3], dst_ref=own_part(p), send_sem=ag2_s.at[p], recv_sem=ag2_r.at[p],
            device_id={"tp": peer(j)})

    def feed(p, lo, hi, between=None, after=()):
        p2, s2 = passes[4 * p:4 * p + 2]
        count = (hi - lo) * CH
        with jax.named_scope("ag_wait"):
            for c in range(lo, hi):
                all_of(rbuf.at[c], ag_r.at[c])

        def h_block(j):
            return hbuf[lo:hi, j].astype(F32).reshape(count, blk)

        with jax.named_scope("feed"):
            total = None
            for j in range(n):
                hj = h_block(j)
                t = jnp.sum(hj * hj, -1, keepdims=True)
                total = t if total is None else total + t
            scale = lax.rsqrt(total * (1.0 / d) + 1e-6)
            at_rows = slice(lo * CH, hi * CH)
            for j in range(n):
                hj = h_block(j)
                for i in range(blk // 128):
                    g = j * (blk // 128) + i
                    bbuf[at_rows, 128 * g:128 * g + 128] = (hj[:, 128 * i:128 * i + 128] * scale * gmv[g:g + 1]).astype(BF16)
        if p == 0:
            with jax.named_scope("w_wait"):
                for cp in third[:4]:
                    cp.wait()
        with jax.named_scope("mlp"):
            hidden = []
            for f in range(wg.shape[1] // 256):
                at = slice(256 * f, 256 * f + 256)
                gate = dot(bbuf[at_rows, :], wg[:, at])
                up = dot(bbuf[at_rows, :], wu[:, at])
                hidden.append((jax.nn.silu(gate) * up).astype(BF16))
            hidden = jnp.concatenate(hidden, 1)
        if between is not None:
            finish(between)
        if p == 0:
            with jax.named_scope("w_wait"):
                for cp in third[4:]:
                    cp.wait()
        with jax.named_scope("down"):
            for j in range(n):
                part = dot(hidden, wd[:, blk * j:blk * (j + 1)])
                p2[j] = part
                s2[j] = part.astype(BF16)
        for c in after:
            finish(c)
        with jax.named_scope("send2"):
            for j in far_first:
                rs2_copy(p, j).start()

    def finish2(p, lo, hi):
        p2, _, r2, ybuf = passes[4 * p:4 * p + 4]
        with jax.named_scope("rs2_wait"):
            all_of(r2, rs2_r.at[p])
        with jax.named_scope("sum2"):
            total = p2[me]
            for j in range(n - 1):
                total = total + r2[j].astype(F32)
            total = total + hbuf[lo:hi, me].astype(F32).reshape((hi - lo) * CH, blk)
            ybuf[...] = total.astype(BF16)
            own_part(p)[...] = ybuf[...]
            for j in far_first:
                ag2_copy(p, j).start()

    for p, (lo, hi) in enumerate(parts):
        if p == 0:
            feed(p, lo, hi, None, (chunks - 2, chunks - 1))
        else:
            feed(p, lo, hi)
    for p, (lo, hi) in enumerate(parts):
        finish2(p, lo, hi)
    with jax.named_scope("sends_wait"):
        for c in range(chunks):
            all_of(rbuf.at[c], rs_s.at[c])
            all_of(rbuf.at[c], ag_s.at[c])
    for p in range(len(PASSES)):
        r2 = passes[4 * p + 2]
        all_of(r2, rs2_s.at[p])
        all_of(r2, ag2_s.at[p])
        with jax.named_scope("ag2_wait"):
            all_of(r2, ag2_r.at[p])


def put_out(y_ref, out_ref, sem):
    copy = pltpu.make_async_copy(y_ref, out_ref, sem)
    copy.start()
    copy.wait()


def solution(mesh):
    n = mesh.shape["tp"]

    def step(x, k_cache, v_cache, gain_a, wq, wo, gain_m, w_gate, w_up, w_down):
        rows, d = x.shape
        batch, cache, heads, head = k_cache.shape
        ff = w_gate.shape[1]
        chunks, blk = rows // CH, d // n
        half = head // 2
        angle = (cache - 1) * float(THETA) ** (-np.arange(half) / half)
        cos, sin = np.cos(angle), np.sin(angle)
        cs = np.zeros((8, head), np.float32)
        cs[0], cs[1] = np.concatenate([cos, cos]), np.concatenate([-sin, sin])
        keys = k_cache.reshape(batch, cache * heads, head)
        values = v_cache.reshape(batch, cache * heads, head)
        second_half = []
        assert sum(PASSES) == chunks
        for count in (CH * p for p in PASSES):
            second_half += [
                pltpu.VMEM((n, count, blk), F32),
                pltpu.VMEM((n, count, blk), BF16),
                pltpu.VMEM((n - 1, count, blk), BF16),
                pltpu.VMEM((count, blk), BF16),
            ]
        dma = pltpu.SemaphoreType.DMA
        y = pl.pallas_call(
            functools.partial(kernel, n),
            out_shape=pltpu.VMEM((rows, d), BF16),
            in_specs=[pl.BlockSpec(memory_space=pl.ANY)] * 11,
            out_specs=pl.BlockSpec(memory_space=pltpu.VMEM),
            scratch_shapes=[
                pltpu.VMEM((rows, d), BF16),
                pltpu.VMEM((rows, d), F32),
                pltpu.VMEM((d // 128, 128), BF16),
                pltpu.VMEM((d // 128, 128), BF16),
                pltpu.VMEM((8, head), F32),
                pltpu.VMEM(wq.shape, BF16),
                pltpu.VMEM(wo.shape, BF16),
                pltpu.VMEM(w_gate.shape, BF16),
                pltpu.VMEM(w_up.shape, BF16),
                pltpu.VMEM(w_down.shape, BF16),
                pltpu.VMEM((SLOTS, CH, cache * heads, head), BF16),
                pltpu.VMEM((SLOTS, CH, cache * heads, head), BF16),
                pltpu.VMEM((rows // GROUP, heads * GROUP, head), F32),
                pltpu.VMEM((AHEAD, CH // GROUP, 4 * GROUP, cache * heads // 2), F32),
                pltpu.VMEM((chunks, n, CH, blk), F32),
                pltpu.VMEM((chunks, n, CH, blk), BF16),
                pltpu.VMEM((chunks, n - 1, CH, blk), BF16),
                pltpu.VMEM((chunks, n, CH, blk), BF16),
                pltpu.VMEM((rows, d), BF16),
                *second_half,
                dma((12,)), dma((SLOTS,)), dma((SLOTS,)),
                dma((chunks,)), dma((chunks,)), dma((chunks,)), dma((chunks,)),
                *[dma((len(PASSES),))] * 4,
            ],
            compiler_params=pltpu.CompilerParams(
                collective_id=0, has_side_effects=True, vmem_limit_bytes=64336 * 1024),
            name="decoder_layer",
        )(x, keys, values, gain_a.reshape(d // 128, 128), wq, wo, gain_m.reshape(d // 128, 128), w_gate, w_up, w_down, jnp.asarray(cs))
        return pl.pallas_call(
            put_out,
            out_shape=jax.ShapeDtypeStruct((rows, d), BF16),
            in_specs=[pl.BlockSpec(memory_space=pltpu.VMEM)],
            out_specs=pl.BlockSpec(memory_space=pl.ANY),
            scratch_shapes=[dma(())],
            compiler_params=pltpu.CompilerParams(vmem_limit_bytes=1024 * 1024),
            name="put_out",
        )(y)

    states, cache, columns, rows_of = P("dp", None), P("dp", None, "tp", None), P(None, "tp"), P("tp", None)
    return jax.shard_map(
        step,
        mesh=mesh,
        in_specs=(states, cache, cache, P(None), columns, rows_of, P(None), columns, columns, rows_of),
        out_specs=states,
        check_vma=False,
    )
```

```python
import functools

import jax
import jax.numpy as jnp
import numpy as np
from jax import lax
from jax.experimental import pallas as pl
from jax.experimental.pallas import tpu as pltpu
from jax.sharding import PartitionSpec as P

HEAD = 128
THETA = 10000
F32, BF16 = jnp.float32, jnp.bfloat16

CH = 8
SLOTS = 3
AHEAD = 1
LAG = 2
GROUP = 4
PASSES = (4, 2, 2)


def dot(a, b):
    return lax.dot_general(a, b, (((1,), (0,)), ((), ())), preferred_element_type=F32)


def dot_t(a, b):
    return lax.dot_general(a, b, (((1,), (1,)), ((), ())), preferred_element_type=F32)


def kernel(n, x_hbm, k_hbm, v_hbm, ga_hbm, wq_hbm, wo_hbm, gm_hbm, wg_hbm, wu_hbm, wd_hbm, cs_hbm, y_ref,
           xb, xf, ga, gm, cs, wq, wo, wg, wu, wd, kbuf, vbuf, qf, wbuf, pf, sbuf, rbuf, hbuf, bbuf, *rest):
    passes, (sem_in, sem_k, sem_v, rs_s, rs_r, ag_s, ag_r, rs2_s, rs2_r, ag2_s, ag2_r) = rest[:-11], rest[-11:]
    me = lax.axis_index("tp")
    rows, d = xb.shape
    chunks = rows // CH
    blk = d // n
    span = kbuf.shape[2] // 2

    far_first = sorted(range(1, n), key=lambda j: -min(j, n - j))

    def peer(j):
        return lax.rem(me + j, n)

    copy = pltpu.make_async_copy
    first = [copy(x_hbm, xb, sem_v.at[1]), copy(ga_hbm, ga, sem_v.at[2]), copy(cs_hbm, cs, sem_k.at[1]), copy(wq_hbm, wq, sem_k.at[2])]
    second = [copy(wo_hbm, wo, sem_in), copy(gm_hbm, gm, sem_v.at[2])]

    class Halves:
        def __init__(self, src, dst, sem):
            self.src, self.dst, self.sem = src, dst, sem

        def start(self):
            half = self.src.shape[0] // 2
            for part in range(2):
                at = pl.ds(part * half, half)
                copy(self.src.at[at], self.dst.at[at], self.sem).start()

        def wait(self):
            copy(self.src, self.dst, self.sem).wait()

    third = [Halves(wg_hbm, wg, sem_k.at[0]), Halves(wu_hbm, wu, sem_k.at[1]), Halves(wd_hbm, wd, sem_k.at[2])]

    class Fetch:
        def __init__(self, hbm, buf, sem, c):
            self.hbm, self.c, slot = hbm, c, lax.rem(c, SLOTS)
            self.buf, self.sem = buf.at[slot], sem.at[slot]

        def start(self):
            for g in range(0, CH, GROUP):
                pltpu.make_async_copy(self.hbm.at[pl.ds(self.c * CH + g, GROUP)], self.buf.at[pl.ds(g, GROUP)], self.sem).start()

        def wait(self):
            pltpu.make_async_copy(self.hbm.at[pl.ds(self.c * CH, CH)], self.buf, self.sem).wait()

    def fetch_k(c):
        return Fetch(k_hbm, kbuf, sem_k, c)

    def fetch_v(c):
        return Fetch(v_hbm, vbuf, sem_v, c)

    with jax.named_scope("start"):
        for cp in first:
            cp.start()
        fetch_k(0).start()
        barrier = pltpu.get_barrier_semaphore()
        for j in range(1, n):
            pl.semaphore_signal(barrier, inc=1, device_id={"tp": peer(j)})

    with jax.named_scope("wait_x"):
        for cp in first[:3]:
            cp.wait()
    with jax.named_scope("norm"):
        fetch_v(0).start()
        fetch_k(1).start()
        xv = xb[...].astype(F32)
        xf[...] = xv
        scale = lax.rsqrt(jnp.sum(xv * xv, -1, keepdims=True) * (1.0 / d) + 1e-6)
        gav = ga[...].astype(F32)
        for i in range(d // 128):
            at = slice(128 * i, 128 * i + 128)
            bbuf[:, at] = (xf[:, at] * scale * gav[i:i + 1]).astype(BF16)
    with jax.named_scope("wait_wq"):
        first[3].wait()
        for cp in second:
            cp.start()
        fetch_v(1).start()
    with jax.named_scope("qproj"):
        q = dot(bbuf[...], wq[...]).astype(BF16).astype(F32)
        for g in range(2):
            t = q[:, HEAD * g:HEAD * (g + 1)]
            turned = (t * cs[0:1] + pltpu.roll(t, HEAD // 2, 1) * cs[1:2]).astype(BF16).astype(F32)
            for i in range(rows // GROUP):
                qf[i, GROUP * g:GROUP * (g + 1)] = turned[GROUP * i:GROUP * (i + 1)]

    def rs_copy(c, j):
        return pltpu.make_async_remote_copy(
            src_ref=sbuf.at[c, peer(j)], dst_ref=rbuf.at[c, j - 1], send_sem=rs_s, recv_sem=rs_r.at[c],
            device_id={"tp": peer(j)})

    ends = [sum(PASSES[:p + 1]) for p in range(len(PASSES))]
    parts = [(hi - count, hi) for hi, count in zip(ends, PASSES)]

    def pass_of(c):
        return sum((c >= hi) * 1 for hi in ends[:-1])

    def ag_copy(c, j):
        return pltpu.make_async_remote_copy(
            src_ref=hbuf.at[c, me], dst_ref=hbuf.at[c, me], send_sem=ag_s, recv_sem=ag_r.at[pass_of(c)],
            device_id={"tp": peer(j)})

    def all_of(ref, sem):
        pltpu.make_async_copy(ref, ref, sem).wait()

    def finish(c):
        with jax.named_scope("finish_wait"):
            all_of(rbuf.at[c], rs_r.at[c])
        with jax.named_scope("finish"):
            total = pf[c, me]
            for j in range(n - 1):
                total = total + rbuf[c, j].astype(F32)
            total = total + xf[pl.ds(pl.multiple_of(c * CH, CH), CH), pl.ds(pl.multiple_of(me * blk, blk), blk)]
            hbuf[c, me] = total.astype(BF16)
            for j in far_first:
                ag_copy(c, j).start()

    tall = 4 * GROUP
    row = lax.broadcasted_iota(jnp.int32, (tall, 2 * HEAD), 0)
    row_w = lax.broadcasted_iota(jnp.int32, (tall, span), 0)
    col_w = lax.broadcasted_iota(jnp.int32, (tall, span), 1)
    own_head = (col_w % 2) == ((row_w // GROUP) % 2)
    groups = CH // GROUP

    def scored(c, g):
        slot = lax.rem(c, SLOTS)
        qg = qf[c * groups + g]
        zero = jnp.zeros_like(qg)
        base = jnp.concatenate([jnp.concatenate([qg, zero], 1), jnp.concatenate([zero, qg], 1)], 0)
        s = None
        for i in range(GROUP):
            lhs = jnp.where(row % GROUP == i, base, 0.0).astype(BF16)
            at = g * GROUP + i
            t = dot_t(lhs, jnp.concatenate([kbuf[slot, at, :span], kbuf[slot, at, span:]], 1))
            s = t if s is None else s + t
        return s

    def softmaxed(s):
        half = tall // 2
        s = jnp.where(own_head, s * HEAD**-0.5, -jnp.inf)
        m = jnp.max(s, -1, keepdims=True)
        m = jnp.maximum(m[:half], m[half:])
        e = jnp.exp(s - jnp.concatenate([m, m], 0))
        z = jnp.sum(e, -1, keepdims=True)
        z = 1.0 / (z[:half] + z[half:])
        return e * jnp.concatenate([z, z], 0)

    def mixed(c, g, w):
        slot = lax.rem(c, SLOTS)
        o = None
        for i in range(GROUP):
            lhs = jnp.where(row_w % GROUP == i, w, 0.0).astype(BF16)
            at = g * GROUP + i
            t = dot(lhs, jnp.concatenate([vbuf[slot, at, :span], vbuf[slot, at, span:]], 1))
            o = t if o is None else o + t
        return o[:tall // 2, :HEAD] + o[tall // 2:, HEAD:]

    def project(c, o):
        upper = lax.broadcasted_iota(jnp.int32, (CH, HEAD), 0) < GROUP
        head0 = jnp.where(upper, o[0], pltpu.roll(o[1], GROUP, 0))
        head1 = jnp.where(upper, pltpu.roll(o[0], GROUP, 0), o[1])
        seen = jnp.concatenate([head0, head1], 1).astype(BF16)
        term = dot(seen, wo[...])
        for j in range(n):
            part = term[:, blk * j:blk * (j + 1)]
            pf[c, j] = part
            sbuf[c, j] = part.astype(BF16)

    def send(c):
        for j in far_first:
            rs_copy(c, j).start()

    with jax.named_scope("k_wait"):
        fetch_k(0).wait()
        fetch_k(2).start()
    with jax.named_scope("weigh"):
        for g in range(groups):
            wbuf[0, g] = softmaxed(scored(0, g))
    with jax.named_scope("wait_wo"):
        for cp in second:
            cp.wait()
    with jax.named_scope("barrier_wait"):
        pl.semaphore_wait(barrier, n - 1)

    def attend(c, _):
        ready = c - AHEAD
        with jax.named_scope("k_wait"):
            fetch_k(c).wait()
        with jax.named_scope("v_wait"):
            fetch_v(ready).wait()

        @pl.when(c + 1 < chunks)
        def _():
            fetch_v(c + 1).start()

        @pl.when(c + 2 < chunks)
        def _():
            fetch_k(c + 2).start()

        @pl.when(c + 1 == chunks)
        def _():
            for cp in third[:2]:
                cp.start()

        with jax.named_scope("attend"):
            at = lax.rem(c, AHEAD)
            before = [wbuf[at, g] for g in range(groups)]
            scores = [scored(c, g) for g in range(groups)]
            o = [mixed(ready, g, before[g]) for g in range(groups)]
            for g in range(groups):
                wbuf[at, g] = softmaxed(scores[g])
            project(ready, o)
        with jax.named_scope("send"):
            send(ready)

        @pl.when(ready >= LAG)
        def _():
            finish(ready - LAG)

        return 0

    lax.fori_loop(AHEAD, chunks, attend, 0)
    rest_of = range(chunks - AHEAD, chunks)
    with jax.named_scope("v_wait"):
        for c in rest_of:
            fetch_v(c).wait()
        third[2].start()
    with jax.named_scope("mix"):
        o = [[mixed(c, g, wbuf[c % AHEAD, g]) for g in range(groups)] for c in rest_of]
        for c in rest_of:
            project(c, o[c - rest_of[0]])
    with jax.named_scope("send"):
        for c in rest_of:
            send(c)
    finish(chunks - 3)

    gmv = gm[...].astype(F32)

    def rs2_copy(p, j):
        return pltpu.make_async_remote_copy(
            src_ref=passes[4 * p + 1].at[peer(j)], dst_ref=passes[4 * p + 2].at[j - 1], send_sem=rs2_s,
            recv_sem=rs2_r.at[p], device_id={"tp": peer(j)})

    def own_part(p):
        lo, hi = parts[p]
        return y_ref.at[pl.ds(lo * CH, (hi - lo) * CH), pl.ds(pl.multiple_of(me * blk, blk), blk)]

    def ag2_copy(p, j):
        return pltpu.make_async_remote_copy(
            src_ref=passes[4 * p + 3], dst_ref=own_part(p), send_sem=ag2_s, recv_sem=ag2_r.at[p],
            device_id={"tp": peer(j)})

    def feed(p, lo, hi, between=None, after=()):
        p2, s2 = passes[4 * p:4 * p + 2]
        count = (hi - lo) * CH
        with jax.named_scope("ag_wait"):
            all_of(rbuf.at[pl.ds(lo, hi - lo)], ag_r.at[p])

        def h_block(j):
            return hbuf[lo:hi, j].astype(F32).reshape(count, blk)

        with jax.named_scope("feed"):
            total = None
            for j in range(n):
                hj = h_block(j)
                t = jnp.sum(hj * hj, -1, keepdims=True)
                total = t if total is None else total + t
            scale = lax.rsqrt(total * (1.0 / d) + 1e-6)
            at_rows = slice(lo * CH, hi * CH)
            for j in range(n):
                hj = h_block(j)
                for i in range(blk // 128):
                    g = j * (blk // 128) + i
                    bbuf[at_rows, 128 * g:128 * g + 128] = (hj[:, 128 * i:128 * i + 128] * scale * gmv[g:g + 1]).astype(BF16)
        if p == 0:
            with jax.named_scope("w_wait"):
                for cp in third[:2]:
                    cp.wait()
        with jax.named_scope("mlp"):
            hidden = []
            for f in range(wg.shape[1] // 256):
                at = slice(256 * f, 256 * f + 256)
                gate = dot(bbuf[at_rows, :], wg[:, at])
                up = dot(bbuf[at_rows, :], wu[:, at])
                hidden.append((jax.nn.silu(gate) * up).astype(BF16))
            hidden = jnp.concatenate(hidden, 1)
        if between is not None:
            finish(between)
        if p == 0:
            with jax.named_scope("w_wait"):
                third[2].wait()
        with jax.named_scope("down"):
            for j in range(n):
                part = dot(hidden, wd[:, blk * j:blk * (j + 1)])
                p2[j] = part
                s2[j] = part.astype(BF16)
        for c in after:
            finish(c)
        with jax.named_scope("send2"):
            for j in far_first:
                rs2_copy(p, j).start()

    def finish2(p, lo, hi):
        p2, _, r2, ybuf = passes[4 * p:4 * p + 4]
        with jax.named_scope("rs2_wait"):
            all_of(r2, rs2_r.at[p])
        with jax.named_scope("sum2"):
            total = p2[me]
            for j in range(n - 1):
                total = total + r2[j].astype(F32)
            total = total + hbuf[lo:hi, me].astype(F32).reshape((hi - lo) * CH, blk)
            ybuf[...] = total.astype(BF16)
            own_part(p)[...] = ybuf[...]
            for j in far_first:
                ag2_copy(p, j).start()

    for p, (lo, hi) in enumerate(parts):
        if p == 0:
            feed(p, lo, hi, None, (chunks - 2, chunks - 1))
        else:
            feed(p, lo, hi)
    for p, (lo, hi) in enumerate(parts):
        finish2(p, lo, hi)
    with jax.named_scope("sends_wait"):
        for sem in (rs_s, ag_s, rs2_s, ag2_s):
            all_of(rbuf, sem)
    for p in range(len(PASSES)):
        with jax.named_scope("ag2_wait"):
            all_of(passes[4 * p + 2], ag2_r.at[p])


def put_out(y_ref, out_ref, sem):
    copy = pltpu.make_async_copy(y_ref, out_ref, sem)
    copy.start()
    copy.wait()


def solution(mesh):
    n = mesh.shape["tp"]

    def step(x, k_cache, v_cache, gain_a, wq, wo, gain_m, w_gate, w_up, w_down):
        rows, d = x.shape
        batch, cache, heads, head = k_cache.shape
        ff = w_gate.shape[1]
        chunks, blk = rows // CH, d // n
        half = head // 2
        angle = (cache - 1) * float(THETA) ** (-np.arange(half) / half)
        cos, sin = np.cos(angle), np.sin(angle)
        cs = np.zeros((8, head), np.float32)
        cs[0], cs[1] = np.concatenate([cos, cos]), np.concatenate([-sin, sin])
        keys = k_cache.reshape(batch, cache * heads, head)
        values = v_cache.reshape(batch, cache * heads, head)
        second_half = []
        assert sum(PASSES) == chunks
        for count in (CH * p for p in PASSES):
            second_half += [
                pltpu.VMEM((n, count, blk), F32),
                pltpu.VMEM((n, count, blk), BF16),
                pltpu.VMEM((n - 1, count, blk), BF16),
                pltpu.VMEM((count, blk), BF16),
            ]
        dma = pltpu.SemaphoreType.DMA
        y = pl.pallas_call(
            functools.partial(kernel, n),
            out_shape=pltpu.VMEM((rows, d), BF16),
            in_specs=[pl.BlockSpec(memory_space=pl.ANY)] * 11,
            out_specs=pl.BlockSpec(memory_space=pltpu.VMEM),
            scratch_shapes=[
                pltpu.VMEM((rows, d), BF16),
                pltpu.VMEM((rows, d), F32),
                pltpu.VMEM((d // 128, 128), BF16),
                pltpu.VMEM((d // 128, 128), BF16),
                pltpu.VMEM((8, head), F32),
                pltpu.VMEM(wq.shape, BF16),
                pltpu.VMEM(wo.shape, BF16),
                pltpu.VMEM(w_gate.shape, BF16),
                pltpu.VMEM(w_up.shape, BF16),
                pltpu.VMEM(w_down.shape, BF16),
                pltpu.VMEM((SLOTS, CH, cache * heads, head), BF16),
                pltpu.VMEM((SLOTS, CH, cache * heads, head), BF16),
                pltpu.VMEM((rows // GROUP, heads * GROUP, head), F32),
                pltpu.VMEM((AHEAD, CH // GROUP, 4 * GROUP, cache * heads // 2), F32),
                pltpu.VMEM((chunks, n, CH, blk), F32),
                pltpu.VMEM((chunks, n, CH, blk), BF16),
                pltpu.VMEM((chunks, n - 1, CH, blk), BF16),
                pltpu.VMEM((chunks, n, CH, blk), BF16),
                pltpu.VMEM((rows, d), BF16),
                *second_half,
                dma(()), dma((SLOTS,)), dma((SLOTS,)),
                dma(()), dma((chunks,)), dma(()), *[dma((len(PASSES),)), dma(())] * 2, dma((len(PASSES),)),
            ],
            compiler_params=pltpu.CompilerParams(
                collective_id=0, has_side_effects=True, vmem_limit_bytes=64336 * 1024),
            name="decoder_layer",
        )(x, keys, values, gain_a.reshape(d // 128, 128), wq, wo, gain_m.reshape(d // 128, 128), w_gate, w_up, w_down, jnp.asarray(cs))
        return pl.pallas_call(
            put_out,
            out_shape=jax.ShapeDtypeStruct((rows, d), BF16),
            in_specs=[pl.BlockSpec(memory_space=pltpu.VMEM)],
            out_specs=pl.BlockSpec(memory_space=pl.ANY),
            scratch_shapes=[dma(())],
            compiler_params=pltpu.CompilerParams(vmem_limit_bytes=1024 * 1024),
            name="put_out",
        )(y)

    states, cache, columns, rows_of = P("dp", None), P("dp", None, "tp", None), P(None, "tp"), P("tp", None)
    return jax.shard_map(
        step,
        mesh=mesh,
        in_specs=(states, cache, cache, P(None), columns, rows_of, P(None), columns, columns, rows_of),
        out_specs=states,
        check_vma=False,
    )
```

```python
import functools

import jax
import jax.numpy as jnp
import numpy as np
from jax import lax
from jax.experimental import pallas as pl
from jax.experimental.pallas import tpu as pltpu
from jax.sharding import PartitionSpec as P

HEAD = 128
THETA = 10000
F32, BF16 = jnp.float32, jnp.bfloat16

CH = 8
SLOTS = 3
LAG = 2
GROUP = 4
PASSES = (4, 2, 2)


def dot(a, b):
    return lax.dot_general(a, b, (((1,), (0,)), ((), ())), preferred_element_type=F32)


def dot_t(a, b):
    return lax.dot_general(a, b, (((1,), (1,)), ((), ())), preferred_element_type=F32)


def kernel(n, x_hbm, k_hbm, v_hbm, ga_hbm, wq_hbm, wo_hbm, gm_hbm, wg_hbm, wu_hbm, wd_hbm, cs_hbm, y_ref,
           xb, xf, ga, gm, cs, wq, wo, wg, wu, wd, kbuf, vbuf, qf, wbuf, pf, sbuf, rbuf, hbuf, bbuf, *rest):
    passes, (sem_in, sem_k, sem_v, rs_s, rs_r, ag_s, ag_r, rs2_s, rs2_r, ag2_s, ag2_r) = rest[:-11], rest[-11:]
    me = lax.axis_index("tp")
    rows, d = xb.shape
    chunks = rows // CH
    blk = d // n
    span = kbuf.shape[2] // 2

    far_first = sorted(range(1, n), key=lambda j: -min(j, n - j))

    def peer(j):
        return lax.rem(me + j, n)

    copy = pltpu.make_async_copy
    first = [copy(x_hbm, xb, sem_v.at[1]), copy(ga_hbm, ga, sem_v.at[2]), copy(cs_hbm, cs, sem_k.at[1]), copy(wq_hbm, wq, sem_k.at[2])]
    second = [copy(wo_hbm, wo, sem_in), copy(gm_hbm, gm, sem_v.at[2])]

    class Halves:
        def __init__(self, src, dst, sem):
            self.src, self.dst, self.sem = src, dst, sem

        def start(self):
            half = self.src.shape[0] // 2
            for part in range(2):
                at = pl.ds(part * half, half)
                copy(self.src.at[at], self.dst.at[at], self.sem).start()

        def wait(self):
            copy(self.src, self.dst, self.sem).wait()

    third = [Halves(wg_hbm, wg, sem_k.at[0]), Halves(wu_hbm, wu, sem_k.at[1]), Halves(wd_hbm, wd, sem_k.at[2])]

    class Fetch:
        def __init__(self, hbm, buf, sem, c):
            self.hbm, self.c, slot = hbm, c, lax.rem(c, SLOTS)
            self.buf, self.sem = buf.at[slot], sem.at[slot]

        def start(self):
            for g in range(0, CH, GROUP):
                pltpu.make_async_copy(self.hbm.at[pl.ds(self.c * CH + g, GROUP)], self.buf.at[pl.ds(g, GROUP)], self.sem).start()

        def wait(self):
            pltpu.make_async_copy(self.hbm.at[pl.ds(self.c * CH, CH)], self.buf, self.sem).wait()

    def fetch_k(c):
        return Fetch(k_hbm, kbuf, sem_k, c)

    def fetch_v(c):
        return Fetch(v_hbm, vbuf, sem_v, c)

    with jax.named_scope("start"):
        for cp in first:
            cp.start()
        fetch_k(0).start()
        barrier = pltpu.get_barrier_semaphore()
        for j in range(1, n):
            pl.semaphore_signal(barrier, inc=1, device_id={"tp": peer(j)})

    with jax.named_scope("wait_x"):
        for cp in first[:3]:
            cp.wait()
    with jax.named_scope("norm"):
        fetch_v(0).start()
        fetch_k(1).start()
        xv = xb[...].astype(F32)
        xf[...] = xv
        scale = lax.rsqrt(jnp.sum(xv * xv, -1, keepdims=True) * (1.0 / d) + 1e-6)
        gav = ga[...].astype(F32)
        for i in range(d // 128):
            at = slice(128 * i, 128 * i + 128)
            bbuf[:, at] = (xf[:, at] * scale * gav[i:i + 1]).astype(BF16)
    with jax.named_scope("wait_wq"):
        first[3].wait()
        for cp in second:
            cp.start()
        fetch_v(1).start()
    with jax.named_scope("qproj"):
        q = dot(bbuf[...], wq[...]).astype(BF16).astype(F32)
        for g in range(2):
            t = q[:, HEAD * g:HEAD * (g + 1)]
            turned = (t * cs[0:1] + pltpu.roll(t, HEAD // 2, 1) * cs[1:2]).astype(BF16).astype(F32)
            for i in range(rows // GROUP):
                qf[i, GROUP * g:GROUP * (g + 1)] = turned[GROUP * i:GROUP * (i + 1)]

    def rs_copy(c, j):
        return pltpu.make_async_remote_copy(
            src_ref=sbuf.at[c, peer(j)], dst_ref=rbuf.at[c, j - 1], send_sem=rs_s, recv_sem=rs_r.at[c],
            device_id={"tp": peer(j)})

    ends = [sum(PASSES[:p + 1]) for p in range(len(PASSES))]
    parts = [(hi - count, hi) for hi, count in zip(ends, PASSES)]

    def pass_of(c):
        return sum((c >= hi) * 1 for hi in ends[:-1])

    def ag_copy(c, j):
        return pltpu.make_async_remote_copy(
            src_ref=hbuf.at[c, me], dst_ref=hbuf.at[c, me], send_sem=ag_s, recv_sem=ag_r.at[pass_of(c)],
            device_id={"tp": peer(j)})

    def all_of(ref, sem):
        pltpu.make_async_copy(ref, ref, sem).wait()

    def finish(c):
        with jax.named_scope("finish_wait"):
            all_of(rbuf.at[c], rs_r.at[c])
        with jax.named_scope("finish"):
            total = pf[c, me]
            for j in range(n - 1):
                total = total + rbuf[c, j].astype(F32)
            total = total + xf[pl.ds(pl.multiple_of(c * CH, CH), CH), pl.ds(pl.multiple_of(me * blk, blk), blk)]
            hbuf[c, me] = total.astype(BF16)
            for j in far_first:
                ag_copy(c, j).start()

    tall = 4 * GROUP
    row = lax.broadcasted_iota(jnp.int32, (tall, 2 * HEAD), 0)
    row_w = lax.broadcasted_iota(jnp.int32, (tall, span), 0)
    col_w = lax.broadcasted_iota(jnp.int32, (tall, span), 1)
    own_head = (col_w % 2) == ((row_w // GROUP) % 2)
    groups = CH // GROUP

    def scored(c, g):
        slot = lax.rem(c, SLOTS)
        qg = qf[c * groups + g]
        zero = jnp.zeros_like(qg)
        base = jnp.concatenate([jnp.concatenate([qg, zero], 1), jnp.concatenate([zero, qg], 1)], 0)
        s = None
        for i in range(GROUP):
            lhs = jnp.where(row % GROUP == i, base, 0.0).astype(BF16)
            at = g * GROUP + i
            t = dot_t(lhs, jnp.concatenate([kbuf[slot, at, :span], kbuf[slot, at, span:]], 1))
            s = t if s is None else s + t
        return s

    def softmaxed(s):
        half = tall // 2
        s = jnp.where(own_head, s * HEAD**-0.5, -jnp.inf)
        m = jnp.max(s, -1, keepdims=True)
        m = jnp.maximum(m[:half], m[half:])
        e = jnp.exp(s - jnp.concatenate([m, m], 0))
        z = jnp.sum(e, -1, keepdims=True)
        z = 1.0 / (z[:half] + z[half:])
        return e * jnp.concatenate([z, z], 0)

    def mixed(c, g, w):
        slot = lax.rem(c, SLOTS)
        o = None
        for i in range(GROUP):
            lhs = jnp.where(row_w % GROUP == i, w, 0.0).astype(BF16)
            at = g * GROUP + i
            t = dot(lhs, jnp.concatenate([vbuf[slot, at, :span], vbuf[slot, at, span:]], 1))
            o = t if o is None else o + t
        return o[:tall // 2, :HEAD] + o[tall // 2:, HEAD:]

    def project(*made):
        upper = lax.broadcasted_iota(jnp.int32, (CH, HEAD), 0) < GROUP
        seen = []
        for _, o in made:
            head0 = jnp.where(upper, o[0], pltpu.roll(o[1], GROUP, 0))
            head1 = jnp.where(upper, pltpu.roll(o[0], GROUP, 0), o[1])
            seen.append(jnp.concatenate([head0, head1], 1))
        term = dot(jnp.concatenate(seen, 0).astype(BF16), wo[...])
        for i, (c, _) in enumerate(made):
            for j in range(n):
                part = term[CH * i:CH * (i + 1), blk * j:blk * (j + 1)]
                pf[c, j] = part
                sbuf[c, j] = part.astype(BF16)

    def send(c):
        for j in far_first:
            rs_copy(c, j).start()

    with jax.named_scope("k_wait"):
        fetch_k(0).wait()
        fetch_k(2).start()
    with jax.named_scope("weigh"):
        for g in range(groups):
            wbuf[g] = softmaxed(scored(0, g))
    with jax.named_scope("wait_wo"):
        for cp in second:
            cp.wait()
    with jax.named_scope("barrier_wait"):
        pl.semaphore_wait(barrier, n - 1)

    def attend(c, _):
        ready = c - 1
        with jax.named_scope("k_wait"):
            fetch_k(c).wait()
        with jax.named_scope("v_wait"):
            fetch_v(ready).wait()

        fetch_v(c + 1).start()

        @pl.when(c + 2 < chunks)
        def _():
            fetch_k(c + 2).start()

        with jax.named_scope("attend"):
            before = [wbuf[g] for g in range(groups)]
            scores = [scored(c, g) for g in range(groups)]
            o = [mixed(ready, g, before[g]) for g in range(groups)]
            for g in range(groups):
                wbuf[g] = softmaxed(scores[g])
            project((ready, o))
        with jax.named_scope("send"):
            send(ready)

        @pl.when(ready >= LAG)
        def _():
            finish(ready - LAG)

        return 0

    lax.fori_loop(1, chunks - 1, attend, 0)

    c = chunks - 1
    with jax.named_scope("k_wait"):
        fetch_k(c).wait()
        fetch_v(c - 1).wait()
        for cp in third[:2]:
            cp.start()
    with jax.named_scope("attend"):
        before = [wbuf[g] for g in range(groups)]
        scores = [scored(c, g) for g in range(groups)]
        early = [mixed(c - 1, g, before[g]) for g in range(groups)]
        for g in range(groups):
            wbuf[g] = softmaxed(scores[g])
    with jax.named_scope("v_wait"):
        fetch_v(c).wait()
        third[2].start()
    with jax.named_scope("mix"):
        project((c - 1, early), (c, [mixed(c, g, wbuf[g]) for g in range(groups)]))
    with jax.named_scope("send"):
        send(c - 1)
        send(c)
    finish(c - 1 - LAG)
    finish(c - LAG)

    gmv = gm[...].astype(F32)

    def rs2_copy(p, j):
        return pltpu.make_async_remote_copy(
            src_ref=passes[4 * p + 1].at[j - 1], dst_ref=passes[4 * p + 2].at[j - 1], send_sem=rs2_s,
            recv_sem=rs2_r.at[p], device_id={"tp": peer(j)})

    def own_part(p):
        lo, hi = parts[p]
        return y_ref.at[pl.ds(lo * CH, (hi - lo) * CH), pl.ds(pl.multiple_of(me * blk, blk), blk)]

    def ag2_copy(p, j):
        return pltpu.make_async_remote_copy(
            src_ref=passes[4 * p + 3], dst_ref=own_part(p), send_sem=ag2_s, recv_sem=ag2_r.at[p],
            device_id={"tp": peer(j)})

    def feed(p, lo, hi, between=None, after=()):
        p2, s2 = passes[4 * p:4 * p + 2]
        count = (hi - lo) * CH
        with jax.named_scope("ag_wait"):
            all_of(rbuf.at[pl.ds(lo, hi - lo)], ag_r.at[p])

        def h_block(j):
            return hbuf[lo:hi, j].astype(F32).reshape(count, blk)

        with jax.named_scope("feed"):
            total = None
            for j in range(n):
                hj = h_block(j)
                t = jnp.sum(hj * hj, -1, keepdims=True)
                total = t if total is None else total + t
            scale = lax.rsqrt(total * (1.0 / d) + 1e-6)
            at_rows = slice(lo * CH, hi * CH)
            for j in range(n):
                hj = h_block(j)
                for i in range(blk // 128):
                    g = j * (blk // 128) + i
                    bbuf[at_rows, 128 * g:128 * g + 128] = (hj[:, 128 * i:128 * i + 128] * scale * gmv[g:g + 1]).astype(BF16)
        if p == 0:
            with jax.named_scope("w_wait"):
                for cp in third[:2]:
                    cp.wait()
        with jax.named_scope("mlp"):
            hidden = []
            for f in range(wg.shape[1] // 256):
                at = slice(256 * f, 256 * f + 256)
                gate = dot(bbuf[at_rows, :], wg[:, at])
                up = dot(bbuf[at_rows, :], wu[:, at])
                hidden.append((jax.nn.silu(gate) * up).astype(BF16))
            hidden = jnp.concatenate(hidden, 1)
        if between is not None:
            finish(between)
        if p == 0:
            with jax.named_scope("w_wait"):
                third[2].wait()
        order = far_first + [0]
        cut = 3 if p == len(PASSES) - 1 else n
        for some in (order[:cut], order[cut:]):
            with jax.named_scope("down"):
                for j in some:
                    part = dot(hidden, wd[:, pl.ds(pl.multiple_of(peer(j) * blk, blk), blk)])
                    if j == 0:
                        p2[...] = part
                    else:
                        s2[j - 1] = part.astype(BF16)
            if cut == n:
                for c in after:
                    finish(c)
            with jax.named_scope("send2"):
                for j in some:
                    if j > 0:
                        rs2_copy(p, j).start()
            if cut == n:
                break

    def finish2(p, lo, hi):
        p2, _, r2, ybuf = passes[4 * p:4 * p + 4]
        with jax.named_scope("rs2_wait"):
            all_of(r2, rs2_r.at[p])
        with jax.named_scope("sum2"):
            total = p2[...]
            for j in range(n - 1):
                total = total + r2[j].astype(F32)
            total = total + hbuf[lo:hi, me].astype(F32).reshape((hi - lo) * CH, blk)
            ybuf[...] = total.astype(BF16)
            own_part(p)[...] = ybuf[...]
            for j in far_first:
                ag2_copy(p, j).start()

    for p, (lo, hi) in enumerate(parts):
        if p == 0:
            feed(p, lo, hi, None, (chunks - 2, chunks - 1))
        else:
            feed(p, lo, hi)
    for p, (lo, hi) in enumerate(parts):
        finish2(p, lo, hi)
    with jax.named_scope("sends_wait"):
        for sem in (rs_s, ag_s, rs2_s, ag2_s):
            all_of(rbuf, sem)
    for p in range(len(PASSES)):
        with jax.named_scope("ag2_wait"):
            all_of(passes[4 * p + 2], ag2_r.at[p])


def put_out(y_ref, out_ref, sem):
    copy = pltpu.make_async_copy(y_ref, out_ref, sem)
    copy.start()
    copy.wait()


def solution(mesh):
    n = mesh.shape["tp"]

    def step(x, k_cache, v_cache, gain_a, wq, wo, gain_m, w_gate, w_up, w_down):
        rows, d = x.shape
        batch, cache, heads, head = k_cache.shape
        ff = w_gate.shape[1]
        chunks, blk = rows // CH, d // n
        half = head // 2
        angle = (cache - 1) * float(THETA) ** (-np.arange(half) / half)
        cos, sin = np.cos(angle), np.sin(angle)
        cs = np.zeros((8, head), np.float32)
        cs[0], cs[1] = np.concatenate([cos, cos]), np.concatenate([-sin, sin])
        keys = k_cache.reshape(batch, cache * heads, head)
        values = v_cache.reshape(batch, cache * heads, head)
        second_half = []
        assert sum(PASSES) == chunks
        for count in (CH * p for p in PASSES):
            second_half += [
                pltpu.VMEM((count, blk), F32),
                pltpu.VMEM((n - 1, count, blk), BF16),
                pltpu.VMEM((n - 1, count, blk), BF16),
                pltpu.VMEM((count, blk), BF16),
            ]
        dma = pltpu.SemaphoreType.DMA
        y = pl.pallas_call(
            functools.partial(kernel, n),
            out_shape=pltpu.VMEM((rows, d), BF16),
            in_specs=[pl.BlockSpec(memory_space=pl.ANY)] * 11,
            out_specs=pl.BlockSpec(memory_space=pltpu.VMEM),
            scratch_shapes=[
                pltpu.VMEM((rows, d), BF16),
                pltpu.VMEM((rows, d), F32),
                pltpu.VMEM((d // 128, 128), BF16),
                pltpu.VMEM((d // 128, 128), BF16),
                pltpu.VMEM((8, head), F32),
                pltpu.VMEM(wq.shape, BF16),
                pltpu.VMEM(wo.shape, BF16),
                pltpu.VMEM(w_gate.shape, BF16),
                pltpu.VMEM(w_up.shape, BF16),
                pltpu.VMEM(w_down.shape, BF16),
                pltpu.VMEM((SLOTS, CH, cache * heads, head), BF16),
                pltpu.VMEM((SLOTS, CH, cache * heads, head), BF16),
                pltpu.VMEM((rows // GROUP, heads * GROUP, head), F32),
                pltpu.VMEM((CH // GROUP, 4 * GROUP, cache * heads // 2), F32),
                pltpu.VMEM((chunks, n, CH, blk), F32),
                pltpu.VMEM((chunks, n, CH, blk), BF16),
                pltpu.VMEM((chunks, n - 1, CH, blk), BF16),
                pltpu.VMEM((chunks, n, CH, blk), BF16),
                pltpu.VMEM((rows, d), BF16),
                *second_half,
                dma(()), dma((SLOTS,)), dma((SLOTS,)),
                dma(()), dma((chunks,)), dma(()), *[dma((len(PASSES),)), dma(())] * 2, dma((len(PASSES),)),
            ],
            compiler_params=pltpu.CompilerParams(
                collective_id=0, has_side_effects=True, vmem_limit_bytes=64336 * 1024),
            name="decoder_layer",
        )(x, keys, values, gain_a.reshape(d // 128, 128), wq, wo, gain_m.reshape(d // 128, 128), w_gate, w_up, w_down, jnp.asarray(cs))
        return pl.pallas_call(
            put_out,
            out_shape=jax.ShapeDtypeStruct((rows, d), BF16),
            in_specs=[pl.BlockSpec(memory_space=pltpu.VMEM)],
            out_specs=pl.BlockSpec(memory_space=pl.ANY),
            scratch_shapes=[dma(())],
            compiler_params=pltpu.CompilerParams(vmem_limit_bytes=1024 * 1024),
            name="put_out",
        )(y)

    states, cache, columns, rows_of = P("dp", None), P("dp", None, "tp", None), P(None, "tp"), P("tp", None)
    return jax.shard_map(
        step,
        mesh=mesh,
        in_specs=(states, cache, cache, P(None), columns, rows_of, P(None), columns, columns, rows_of),
        out_specs=states,
        check_vma=False,
    )
```

```python
import functools

import jax
import jax.numpy as jnp
import numpy as np
from jax import lax
from jax.experimental import pallas as pl
from jax.experimental.pallas import tpu as pltpu
from jax.sharding import PartitionSpec as P

HEAD = 128
THETA = 10000
F32, BF16 = jnp.float32, jnp.bfloat16

CH = 8
SLOTS = 3
LAG = 2
GROUP = 4
PASSES = (4, 2, 2)


def dot(a, b):
    return lax.dot_general(a, b, (((1,), (0,)), ((), ())), preferred_element_type=F32)


def dot_t(a, b):
    return lax.dot_general(a, b, (((1,), (1,)), ((), ())), preferred_element_type=F32)


def kernel(n, x_hbm, k_hbm, v_hbm, ga_hbm, wq_hbm, wo_hbm, gm_hbm, wg_hbm, wu_hbm, wd_hbm, cs_hbm, y_ref,
           xb, xf, ga, gm, cs, wq, wo, wg, wu, wd, kbuf, vbuf, qf, wbuf, pf, sbuf, rbuf, hbuf, bbuf, *rest):
    passes, (sem_in, sem_k, sem_v, rs_s, rs_r, ag_s, ag_r, rs2_s, rs2_r, ag2_s, ag2_r) = rest[:-11], rest[-11:]
    me = lax.axis_index("tp")
    rows, d = xb.shape
    chunks = rows // CH
    blk = d // n
    span = kbuf.shape[2] // 2

    far_first = sorted(range(1, n), key=lambda j: -min(j, n - j))

    def peer(j):
        return lax.rem(me + j, n)

    copy = pltpu.make_async_copy
    first = [copy(x_hbm, xb, sem_v.at[1]), copy(ga_hbm, ga, sem_v.at[2]), copy(cs_hbm, cs, sem_k.at[1]), copy(wq_hbm, wq, sem_k.at[2])]
    second = [copy(wo_hbm, wo, sem_in), copy(gm_hbm, gm, sem_v.at[2])]

    class Halves:
        def __init__(self, src, dst, sem):
            self.src, self.dst, self.sem = src, dst, sem

        def start(self):
            half = self.src.shape[0] // 2
            for part in range(2):
                at = pl.ds(part * half, half)
                copy(self.src.at[at], self.dst.at[at], self.sem).start()

        def wait(self):
            copy(self.src, self.dst, self.sem).wait()

    third = [Halves(wg_hbm, wg, sem_k.at[0]), Halves(wu_hbm, wu, sem_k.at[1]), Halves(wd_hbm, wd, sem_k.at[2])]

    class Fetch:
        def __init__(self, hbm, buf, sem, c):
            self.hbm, self.c, slot = hbm, c, lax.rem(c, SLOTS)
            self.buf, self.sem = buf.at[slot], sem.at[slot]

        def start(self):
            for g in range(0, CH, GROUP):
                pltpu.make_async_copy(self.hbm.at[pl.ds(self.c * CH + g, GROUP)], self.buf.at[pl.ds(g, GROUP)], self.sem).start()

        def wait(self):
            pltpu.make_async_copy(self.hbm.at[pl.ds(self.c * CH, CH)], self.buf, self.sem).wait()

    def fetch_k(c):
        return Fetch(k_hbm, kbuf, sem_k, c)

    def fetch_v(c):
        return Fetch(v_hbm, vbuf, sem_v, c)

    with jax.named_scope("start"):
        for cp in first:
            cp.start()
        fetch_k(0).start()
        barrier = pltpu.get_barrier_semaphore()
        for j in range(1, n):
            pl.semaphore_signal(barrier, inc=1, device_id={"tp": peer(j)})

    with jax.named_scope("wait_x"):
        for cp in first[:3]:
            cp.wait()
    with jax.named_scope("norm"):
        fetch_v(0).start()
        fetch_k(1).start()
        xv = xb[...].astype(F32)
        xf[...] = xv
        scale = lax.rsqrt(jnp.sum(xv * xv, -1, keepdims=True) * (1.0 / d) + 1e-6)
        gav = ga[...].astype(F32)
        for i in range(d // 128):
            at = slice(128 * i, 128 * i + 128)
            bbuf[:, at] = (xf[:, at] * scale * gav[i:i + 1]).astype(BF16)
    with jax.named_scope("wait_wq"):
        first[3].wait()
        for cp in second:
            cp.start()
        fetch_v(1).start()
    with jax.named_scope("qproj"):
        q = dot(bbuf[...], wq[...]).astype(BF16).astype(F32)
        for g in range(2):
            t = q[:, HEAD * g:HEAD * (g + 1)]
            turned = (t * cs[0:1] + pltpu.roll(t, HEAD // 2, 1) * cs[1:2]).astype(BF16).astype(F32)
            for i in range(rows // GROUP):
                qf[i, GROUP * g:GROUP * (g + 1)] = turned[GROUP * i:GROUP * (i + 1)]

    def rs_copy(c, j):
        return pltpu.make_async_remote_copy(
            src_ref=sbuf.at[c, peer(j)], dst_ref=rbuf.at[c, j - 1], send_sem=rs_s, recv_sem=rs_r.at[c],
            device_id={"tp": peer(j)})

    ends = [sum(PASSES[:p + 1]) for p in range(len(PASSES))]
    parts = [(hi - count, hi) for hi, count in zip(ends, PASSES)]

    def pass_of(c):
        return sum((c >= hi) * 1 for hi in ends[:-1])

    def ag_copy(c, j):
        return pltpu.make_async_remote_copy(
            src_ref=hbuf.at[c, me], dst_ref=hbuf.at[c, me], send_sem=ag_s, recv_sem=ag_r.at[pass_of(c)],
            device_id={"tp": peer(j)})

    def all_of(ref, sem):
        pltpu.make_async_copy(ref, ref, sem).wait()

    def finish(c):
        with jax.named_scope("finish_wait"):
            all_of(rbuf.at[c], rs_r.at[c])
        with jax.named_scope("finish"):
            total = pf[c, me]
            for j in range(n - 1):
                total = total + rbuf[c, j].astype(F32)
            total = total + xf[pl.ds(pl.multiple_of(c * CH, CH), CH), pl.ds(pl.multiple_of(me * blk, blk), blk)]
            hbuf[c, me] = total.astype(BF16)
            for j in far_first:
                ag_copy(c, j).start()

    late = pl.ds(chunks - 2, 2)

    def finish_late():
        with jax.named_scope("finish_wait"):
            all_of(rbuf.at[late], rs_r.at[chunks - 2])
        with jax.named_scope("finish"):
            for c in (chunks - 2, chunks - 1):
                total = pf[c, me]
                for j in range(n - 1):
                    total = total + rbuf[c, j].astype(F32)
                total = total + xf[c * CH:(c + 1) * CH, pl.ds(pl.multiple_of(me * blk, blk), blk)]
                hbuf[c, me] = total.astype(BF16)
            for j in far_first:
                pltpu.make_async_remote_copy(
                    src_ref=hbuf.at[late, me], dst_ref=hbuf.at[late, me], send_sem=ag_s,
                    recv_sem=ag_r.at[len(PASSES) - 1], device_id={"tp": peer(j)}).start()

    def send_late():
        for j in far_first:
            pltpu.make_async_remote_copy(
                src_ref=sbuf.at[late, peer(j)], dst_ref=rbuf.at[late, j - 1], send_sem=rs_s,
                recv_sem=rs_r.at[chunks - 2], device_id={"tp": peer(j)}).start()

    tall = 4 * GROUP
    row = lax.broadcasted_iota(jnp.int32, (tall, 2 * HEAD), 0)
    row_w = lax.broadcasted_iota(jnp.int32, (tall, span), 0)
    col_w = lax.broadcasted_iota(jnp.int32, (tall, span), 1)
    own_head = (col_w % 2) == ((row_w // GROUP) % 2)
    groups = CH // GROUP

    def scored(c, g):
        slot = lax.rem(c, SLOTS)
        qg = qf[c * groups + g]
        zero = jnp.zeros_like(qg)
        base = jnp.concatenate([jnp.concatenate([qg, zero], 1), jnp.concatenate([zero, qg], 1)], 0)
        s = None
        for i in range(GROUP):
            lhs = jnp.where(row % GROUP == i, base, 0.0).astype(BF16)
            at = g * GROUP + i
            t = dot_t(lhs, jnp.concatenate([kbuf[slot, at, :span], kbuf[slot, at, span:]], 1))
            s = t if s is None else s + t
        return s

    def softmaxed(s):
        half = tall // 2
        s = jnp.where(own_head, s * HEAD**-0.5, -jnp.inf)
        m = jnp.max(s, -1, keepdims=True)
        m = jnp.maximum(m[:half], m[half:])
        e = jnp.exp(s - jnp.concatenate([m, m], 0))
        z = jnp.sum(e, -1, keepdims=True)
        z = 1.0 / (z[:half] + z[half:])
        return e * jnp.concatenate([z, z], 0)

    def mixed(c, g, w):
        slot = lax.rem(c, SLOTS)
        o = None
        for i in range(GROUP):
            lhs = jnp.where(row_w % GROUP == i, w, 0.0).astype(BF16)
            at = g * GROUP + i
            t = dot(lhs, jnp.concatenate([vbuf[slot, at, :span], vbuf[slot, at, span:]], 1))
            o = t if o is None else o + t
        return o[:tall // 2, :HEAD] + o[tall // 2:, HEAD:]

    def project(*made):
        upper = lax.broadcasted_iota(jnp.int32, (CH, HEAD), 0) < GROUP
        seen = []
        for _, o in made:
            head0 = jnp.where(upper, o[0], pltpu.roll(o[1], GROUP, 0))
            head1 = jnp.where(upper, pltpu.roll(o[0], GROUP, 0), o[1])
            seen.append(jnp.concatenate([head0, head1], 1))
        term = dot(jnp.concatenate(seen, 0).astype(BF16), wo[...])
        for i, (c, _) in enumerate(made):
            for j in range(n):
                part = term[CH * i:CH * (i + 1), blk * j:blk * (j + 1)]
                pf[c, j] = part
                sbuf[c, j] = part.astype(BF16)

    def send(c):
        for j in far_first:
            rs_copy(c, j).start()

    with jax.named_scope("k_wait"):
        fetch_k(0).wait()
        fetch_k(2).start()
    with jax.named_scope("weigh"):
        for g in range(groups):
            wbuf[g] = softmaxed(scored(0, g))
    with jax.named_scope("wait_wo"):
        for cp in second:
            cp.wait()
    with jax.named_scope("barrier_wait"):
        pl.semaphore_wait(barrier, n - 1)

    def attend(c, _):
        ready = c - 1
        with jax.named_scope("k_wait"):
            fetch_k(c).wait()
        with jax.named_scope("v_wait"):
            fetch_v(ready).wait()

        fetch_v(c + 1).start()

        @pl.when(c + 2 < chunks)
        def _():
            fetch_k(c + 2).start()

        with jax.named_scope("attend"):
            before = [wbuf[g] for g in range(groups)]
            scores = [scored(c, g) for g in range(groups)]
            o = [mixed(ready, g, before[g]) for g in range(groups)]
            for g in range(groups):
                wbuf[g] = softmaxed(scores[g])
            project((ready, o))
        with jax.named_scope("send"):
            send(ready)

        @pl.when(ready >= LAG)
        def _():
            finish(ready - LAG)

        return 0

    lax.fori_loop(1, chunks - 1, attend, 0)

    c = chunks - 1
    with jax.named_scope("k_wait"):
        fetch_k(c).wait()
        fetch_v(c - 1).wait()
        for cp in third[:2]:
            cp.start()
    with jax.named_scope("attend"):
        before = [wbuf[g] for g in range(groups)]
        scores = [scored(c, g) for g in range(groups)]
        early = [mixed(c - 1, g, before[g]) for g in range(groups)]
        for g in range(groups):
            wbuf[g] = softmaxed(scores[g])
    with jax.named_scope("v_wait"):
        fetch_v(c).wait()
        third[2].start()
    with jax.named_scope("mix"):
        project((c - 1, early), (c, [mixed(c, g, wbuf[g]) for g in range(groups)]))
    with jax.named_scope("send"):
        send_late()
    finish(c - 1 - LAG)
    finish(c - LAG)

    gmv = gm[...].astype(F32)

    def rs2_copy(p, j):
        return pltpu.make_async_remote_copy(
            src_ref=passes[4 * p + 1].at[j - 1], dst_ref=passes[4 * p + 2].at[j - 1], send_sem=rs2_s,
            recv_sem=rs2_r.at[p], device_id={"tp": peer(j)})

    def own_part(p):
        lo, hi = parts[p]
        return y_ref.at[pl.ds(lo * CH, (hi - lo) * CH), pl.ds(pl.multiple_of(me * blk, blk), blk)]

    def ag2_copy(p, j):
        return pltpu.make_async_remote_copy(
            src_ref=passes[4 * p + 3], dst_ref=own_part(p), send_sem=ag2_s, recv_sem=ag2_r.at[p],
            device_id={"tp": peer(j)})

    def feed(p, lo, hi, between=None, after=None):
        p2, s2 = passes[4 * p:4 * p + 2]
        count = (hi - lo) * CH
        with jax.named_scope("ag_wait"):
            all_of(rbuf.at[pl.ds(lo, hi - lo)], ag_r.at[p])

        def h_block(j):
            return hbuf[lo:hi, j].astype(F32).reshape(count, blk)

        with jax.named_scope("feed"):
            total = None
            for j in range(n):
                hj = h_block(j)
                t = jnp.sum(hj * hj, -1, keepdims=True)
                total = t if total is None else total + t
            scale = lax.rsqrt(total * (1.0 / d) + 1e-6)
            at_rows = slice(lo * CH, hi * CH)
            for j in range(n):
                hj = h_block(j)
                for i in range(blk // 128):
                    g = j * (blk // 128) + i
                    bbuf[at_rows, 128 * g:128 * g + 128] = (hj[:, 128 * i:128 * i + 128] * scale * gmv[g:g + 1]).astype(BF16)
        if p == 0:
            with jax.named_scope("w_wait"):
                for cp in third[:2]:
                    cp.wait()
        with jax.named_scope("mlp"):
            hidden = []
            for f in range(wg.shape[1] // 256):
                at = slice(256 * f, 256 * f + 256)
                gate = dot(bbuf[at_rows, :], wg[:, at])
                up = dot(bbuf[at_rows, :], wu[:, at])
                hidden.append((jax.nn.silu(gate) * up).astype(BF16))
            hidden = jnp.concatenate(hidden, 1)
        if between is not None:
            finish(between)
        if p == 0:
            with jax.named_scope("w_wait"):
                third[2].wait()
        order = far_first + [0]
        cut = 3 if p == len(PASSES) - 1 else n
        for some in (order[:cut], order[cut:]):
            with jax.named_scope("down"):
                for j in some:
                    part = dot(hidden, wd[:, pl.ds(pl.multiple_of(peer(j) * blk, blk), blk)])
                    if j == 0:
                        p2[...] = part
                    else:
                        s2[j - 1] = part.astype(BF16)
            if after is not None:
                after()
            with jax.named_scope("send2"):
                for j in some:
                    if j > 0:
                        rs2_copy(p, j).start()
            if cut == n:
                break

    def finish2(p, lo, hi):
        p2, _, r2, ybuf = passes[4 * p:4 * p + 4]
        with jax.named_scope("rs2_wait"):
            all_of(r2, rs2_r.at[p])
        with jax.named_scope("sum2"):
            total = p2[...]
            for j in range(n - 1):
                total = total + r2[j].astype(F32)
            total = total + hbuf[lo:hi, me].astype(F32).reshape((hi - lo) * CH, blk)
            ybuf[...] = total.astype(BF16)
            own_part(p)[...] = ybuf[...]
            for j in far_first:
                ag2_copy(p, j).start()

    for p, (lo, hi) in enumerate(parts):
        if p == 0:
            feed(p, lo, hi, None, finish_late)
        else:
            feed(p, lo, hi)
    for p, (lo, hi) in enumerate(parts):
        finish2(p, lo, hi)
    with jax.named_scope("sends_wait"):
        for sem in (rs_s, ag_s, rs2_s, ag2_s):
            all_of(rbuf, sem)
    for p in range(len(PASSES)):
        with jax.named_scope("ag2_wait"):
            all_of(passes[4 * p + 2], ag2_r.at[p])


def put_out(y_ref, out_ref, sem):
    copy = pltpu.make_async_copy(y_ref, out_ref, sem)
    copy.start()
    copy.wait()


def solution(mesh):
    n = mesh.shape["tp"]

    def step(x, k_cache, v_cache, gain_a, wq, wo, gain_m, w_gate, w_up, w_down):
        rows, d = x.shape
        batch, cache, heads, head = k_cache.shape
        ff = w_gate.shape[1]
        chunks, blk = rows // CH, d // n
        half = head // 2
        angle = (cache - 1) * float(THETA) ** (-np.arange(half) / half)
        cos, sin = np.cos(angle), np.sin(angle)
        cs = np.zeros((8, head), np.float32)
        cs[0], cs[1] = np.concatenate([cos, cos]), np.concatenate([-sin, sin])
        keys = k_cache.reshape(batch, cache * heads, head)
        values = v_cache.reshape(batch, cache * heads, head)
        second_half = []
        assert sum(PASSES) == chunks and PASSES[-1] == 2
        for count in (CH * p for p in PASSES):
            second_half += [
                pltpu.VMEM((count, blk), F32),
                pltpu.VMEM((n - 1, count, blk), BF16),
                pltpu.VMEM((n - 1, count, blk), BF16),
                pltpu.VMEM((count, blk), BF16),
            ]
        dma = pltpu.SemaphoreType.DMA
        y = pl.pallas_call(
            functools.partial(kernel, n),
            out_shape=pltpu.VMEM((rows, d), BF16),
            in_specs=[pl.BlockSpec(memory_space=pl.ANY)] * 11,
            out_specs=pl.BlockSpec(memory_space=pltpu.VMEM),
            scratch_shapes=[
                pltpu.VMEM((rows, d), BF16),
                pltpu.VMEM((rows, d), F32),
                pltpu.VMEM((d // 128, 128), BF16),
                pltpu.VMEM((d // 128, 128), BF16),
                pltpu.VMEM((8, head), F32),
                pltpu.VMEM(wq.shape, BF16),
                pltpu.VMEM(wo.shape, BF16),
                pltpu.VMEM(w_gate.shape, BF16),
                pltpu.VMEM(w_up.shape, BF16),
                pltpu.VMEM(w_down.shape, BF16),
                pltpu.VMEM((SLOTS, CH, cache * heads, head), BF16),
                pltpu.VMEM((SLOTS, CH, cache * heads, head), BF16),
                pltpu.VMEM((rows // GROUP, heads * GROUP, head), F32),
                pltpu.VMEM((CH // GROUP, 4 * GROUP, cache * heads // 2), F32),
                pltpu.VMEM((chunks, n, CH, blk), F32),
                pltpu.VMEM((chunks, n, CH, blk), BF16),
                pltpu.VMEM((chunks, n - 1, CH, blk), BF16),
                pltpu.VMEM((chunks, n, CH, blk), BF16),
                pltpu.VMEM((rows, d), BF16),
                *second_half,
                dma(()), dma((SLOTS,)), dma((SLOTS,)),
                dma(()), dma((chunks - 1,)), dma(()), *[dma((len(PASSES),)), dma(())] * 2, dma((len(PASSES),)),
            ],
            compiler_params=pltpu.CompilerParams(
                collective_id=0, has_side_effects=True, vmem_limit_bytes=64336 * 1024),
            name="decoder_layer",
        )(x, keys, values, gain_a.reshape(d // 128, 128), wq, wo, gain_m.reshape(d // 128, 128), w_gate, w_up, w_down, jnp.asarray(cs))
        return pl.pallas_call(
            put_out,
            out_shape=jax.ShapeDtypeStruct((rows, d), BF16),
            in_specs=[pl.BlockSpec(memory_space=pltpu.VMEM)],
            out_specs=pl.BlockSpec(memory_space=pl.ANY),
            scratch_shapes=[dma(())],
            compiler_params=pltpu.CompilerParams(vmem_limit_bytes=1024 * 1024),
            name="put_out",
        )(y)

    states, cache, columns, rows_of = P("dp", None), P("dp", None, "tp", None), P(None, "tp"), P("tp", None)
    return jax.shard_map(
        step,
        mesh=mesh,
        in_specs=(states, cache, cache, P(None), columns, rows_of, P(None), columns, columns, rows_of),
        out_specs=states,
        check_vma=False,
    )
```
